256 devices in a mesh: cp: 32 (over z_hi, x, core), tp: 8 (over z_lo, y).
Axes of the slice: x: 4, y: 4, z: 8 (z_hi: 4, z_lo: 2; z = z_hi * 2 + z_lo), core: 2. Of those that a mesh axis runs over, the one named last changes fastest.
Arguments:
- hidden: bfloat16 [16384, 4096], P('cp', 'tp'), may hold values from -6 to 6
- norm_gain: float32 [4096], replicated, may hold values from 0.5 to 1.5
- w_query: bfloat16 [4096, 4096], P(None, 'tp'), may hold values from -0.140625 to 0.140625
- w_key: bfloat16 [4096, 1024], P(None, 'tp'), may hold values from -4 to 4
- w_value: bfloat16 [4096, 1024], P(None, 'tp'), may hold values from -0.09375 to 0.09375
- w_out: bfloat16 [4096, 4096], P('tp'), may hold values from -0.5 to 0.5
- doc_ids: int32 [16384], P('cp'), may hold values from 0 to 5, never falling along the last dimension, each value on 1 to 12288 neighbouring positions
Outputs:
- updated: bfloat16 [16384, 4096], P('cp', 'tp')
The draws below stay inside these ranges and needn't reach their ends.
Inputs may be any that keep to these rules, and one draw needn't show every extreme that they name: `doc_ids`: document numbers never fall along the sequence; every document has 1 to 12288 tokens.
All inputs are finite; a program needn't handle non-finite values.
Results may differ from the reference program's by a relative error of at most 0.017.
The reference program's roundings to bfloat16 on the way count: a program that leaves them out, or rounds other values in their place, can miss the bound.
Values may be sent and summed in bfloat16 or wider, within the bound.
A program may use at most 128 MiB of HBM per device.

```python
import math
import jax
import jax.numpy as jnp
import numpy as np
from jax import lax

D = 4096
HEADS = 32
KV_HEADS = 8
HEAD_SIZE = 128
TOK_DEV = 512
DOCS = 6
SEQ = 16384
LONGEST = 12288
N_TP = 8


def query_key_pair(key):
    spread = 1.5 / math.sqrt(D)
    limit = 9.0 / math.sqrt(D)
    base = jax.random.normal(jax.random.fold_in(key, 101), (D, HEADS * HEAD_SIZE), jnp.float32) * spread
    base = jnp.clip(base, -limit, limit)
    other = jax.random.normal(jax.random.fold_in(key, 202), (D, KV_HEADS * HEAD_SIZE), jnp.float32) * spread
    other = jnp.clip(other, -limit, limit)
    return (base, other)


def draw_w_query(key, part):
    base, other = query_key_pair(key)
    return base.astype(jnp.bfloat16)


def draw_w_key(key, part):
    base, other = query_key_pair(key)
    result = other
    return result.astype(jnp.bfloat16)


def block_levels(rng, dims, cuts, low, top_value):
    loudness = 1.0
    for axis_at, shards_of in cuts:
        draws = jax.random.uniform(jax.random.fold_in(jax.random.fold_in(rng, 6), axis_at), (shards_of,), jnp.float32, low / len(cuts), top_value / len(cuts))
        loudness = loudness * jnp.repeat(jnp.exp(draws), dims[axis_at] // shards_of).reshape((-1,) + (1,) * (len(dims) - 1 - axis_at))
    return loudness


def length_profile(amount, total, reach, slope):
    loads = [(1 << 20) // math.isqrt(standing ** slope) + 1 for standing in range(2, amount + 1)]
    rest, given = total - reach - (amount - 1), [1] * (amount - 1)
    while rest > 0:
        free = [i for i in range(amount - 1) if given[i] < reach]
        whole, remaining = sum([loads[i] for i in free]), rest
        for i in free:
            addition = min(reach - given[i], max(1, remaining * loads[i] // whole), rest)
            given[i] = given[i] + addition
            rest = rest - addition
    return np.array([reach] + given)


def uneven(own_key, number_of, total, reach, skew):
    if number_of == 2:
        one = jax.random.randint(own_key, (), max(1, total - reach), min(reach, total - 1) + 1)
        return jnp.stack([one, total - one])
    sizes = jnp.asarray(length_profile(number_of, total, reach, skew), jnp.int32)
    twos = (number_of - 1) // 2
    donor, sink = sizes[1:1 + 2 * twos:2], sizes[2:2 + 2 * twos:2]
    slack = jnp.minimum(donor - 1, reach - sink)
    passed = jax.random.randint(jax.random.fold_in(own_key, 1), (twos,), 0, 1 << 20) % (slack + 1)
    sizes = sizes.at[1:1 + 2 * twos:2].set(donor - passed).at[2:2 + 2 * twos:2].set(sink + passed)
    return sizes[jax.random.permutation(jax.random.fold_in(own_key, 2), number_of)]


def centred(own_key, dims, scale, most, shards=(), held_as=jnp.bfloat16):
    values = scale * jax.random.normal(own_key, dims, jnp.float32)
    if shards:
        values = values * block_levels(own_key, dims, shards, -0.22, 0.18)
    return jnp.clip(values, -most, most).astype(held_as)


def setup_inputs(seed: int = 0) -> dict:
    seeds = jax.random.split(jax.random.key(seed), 8)
    return {
        "hidden": centred(seeds[0], (SEQ, D), 1.0, 6.0, ((0, 32), (1, 8))),
        "norm_gain": jnp.clip(1.0 + 0.1 * jax.random.normal(seeds[1], (D,), jnp.float32), 0.5, 1.5),
        "w_query": draw_w_query(jax.random.fold_in(seeds[7], 71), 0),
        "w_key": draw_w_key(jax.random.fold_in(seeds[7], 71), 0),
        "w_value": centred(seeds[4], (D, KV_HEADS * HEAD_SIZE), D ** -0.5, 0.09375, ((1, 8),)),
        "w_out": centred(seeds[5], (HEADS * HEAD_SIZE, D), (HEADS * HEAD_SIZE // 32) ** -0.5, 0.5, ((0, 8),)),
        "doc_ids": jnp.searchsorted(jnp.cumsum(uneven(seeds[6], DOCS, SEQ, LONGEST, 2)), jnp.arange(SEQ), side="right").astype(jnp.int32),
    }


epsilon = 1e-05
rope_base = 500000.0

def rotate(vectors, positions):
    half = HEAD_SIZE // 2
    freqs = rope_base ** (-jnp.arange(half, dtype=jnp.float32) * 2.0 / HEAD_SIZE)
    angles = positions.astype(jnp.float32)[:, None] * freqs[None, :]
    cosine = jnp.cos(angles)[:, None, :]
    sine = jnp.sin(angles)[:, None, :]
    first = vectors[..., :half]
    second = vectors[..., half:]
    return jnp.concatenate([first * cosine - second * sine, second * cosine + first * sine], axis=-1)

def attend_block(loop_state, query_matrix, query_pos, query_doc, key_matrix, value_matrix, key_pos, key_doc):
    best, total, running_output = loop_state
    logit_matrix = jnp.einsum('ucpm,ycm->cpuy', query_matrix.astype(jnp.float32), key_matrix.astype(jnp.float32)) * HEAD_SIZE ** (-0.5)
    allowed = (key_pos[None, :] <= query_pos[:, None]) & (key_doc[None, :] == query_doc[:, None])
    masked = jnp.where(allowed, logit_matrix, jnp.float32(-1e+30))
    new_best = jnp.maximum(best, lax.optimization_barrier(jnp.max(masked, axis=-1)))
    correction_scale = jnp.exp(best - new_best)
    attention_weights = jnp.where(allowed, jnp.exp(logit_matrix - new_best[..., None]), jnp.float32(0.0))
    total = total * correction_scale + lax.optimization_barrier(jnp.sum(attention_weights, axis=-1))
    rounded_weights = attention_weights.astype(jnp.bfloat16).astype(jnp.float32)
    running_output = running_output * correction_scale[..., None] + jnp.einsum('sfec,csh->sfeh', rounded_weights, value_matrix.astype(jnp.float32))
    return (new_best, total, running_output)

def reference(hidden, norm_gain, w_query, w_key, w_value, w_out, doc_ids):
    seq_len = hidden.shape[0]
    group = HEADS // KV_HEADS
    wide = hidden.astype(jnp.float32)
    inverse_rms = lax.rsqrt(lax.optimization_barrier(jnp.mean(wide * wide, axis=1, keepdims=True)) + epsilon)
    normed = (wide * inverse_rms * norm_gain.astype(jnp.float32)[None, :]).astype(jnp.bfloat16)
    positions = jnp.arange(seq_len, dtype=jnp.int32)
    query_raw = jnp.dot(normed, w_query, preferred_element_type=jnp.float32).reshape(seq_len, HEADS, HEAD_SIZE)
    key_raw = jnp.dot(normed, w_key, preferred_element_type=jnp.float32).reshape(seq_len, KV_HEADS, HEAD_SIZE)
    query_matrix = rotate(query_raw, positions).astype(jnp.bfloat16).reshape(seq_len, KV_HEADS, group, HEAD_SIZE)
    key_matrix = rotate(key_raw, positions).astype(jnp.bfloat16)
    value_matrix = jnp.dot(normed, w_value, preferred_element_type=jnp.float32).astype(jnp.bfloat16).reshape(seq_len, KV_HEADS, HEAD_SIZE)
    block_index = TOK_DEV if TOK_DEV <= 512 else 512
    blocks = seq_len // block_index

    def one_query_block(index):
        start = (index * block_index).astype(jnp.int32)
        query_blk = lax.dynamic_slice_in_dim(query_matrix, start, block_index, 0)
        query_pos = start + jnp.arange(block_index, dtype=jnp.int32)
        query_doc = lax.dynamic_slice_in_dim(doc_ids, start, block_index, 0)

        def loop_body(loop_state, key_block_index):
            key_offset = (key_block_index * block_index).astype(jnp.int32)

            def work(state):
                key_blk = lax.dynamic_slice_in_dim(key_matrix, key_offset, block_index, 0)
                value_blk = lax.dynamic_slice_in_dim(value_matrix, key_offset, block_index, 0)
                key_pos = key_offset + jnp.arange(block_index, dtype=jnp.int32)
                key_doc = lax.dynamic_slice_in_dim(doc_ids, key_offset, block_index, 0)
                return attend_block(state, query_blk, query_pos, query_doc, key_blk, value_blk, key_pos, key_doc)
            return (lax.cond(key_offset <= start + block_index - 1, work, lambda state: state, loop_state), None)
        init = (jnp.full((KV_HEADS, group, block_index), -1e+30, jnp.float32), jnp.zeros((KV_HEADS, group, block_index), jnp.float32), jnp.zeros((KV_HEADS, group, block_index, HEAD_SIZE), jnp.float32))
        final, _ = lax.scan(loop_body, init, jnp.arange(blocks, dtype=jnp.int32))
        result = final[2] / final[1][..., None]
        return jnp.transpose(result, (2, 0, 1, 3)).reshape(block_index, HEADS * HEAD_SIZE).astype(jnp.bfloat16)
    attended = lax.map(one_query_block, jnp.arange(blocks, dtype=jnp.int32)).reshape(seq_len, HEADS * HEAD_SIZE)
    width_cols = HEADS * HEAD_SIZE // N_TP
    mixed = jnp.zeros((seq_len, hidden.shape[1]), jnp.float32)
    for group_index in range(N_TP):
        lower = group_index * width_cols
        partial_sum = jnp.dot(attended[:, lower:lower + width_cols], w_out[lower:lower + width_cols], preferred_element_type=jnp.float32).astype(jnp.bfloat16)
        partial_sum = lax.optimization_barrier(partial_sum)
        mixed = mixed + partial_sum.astype(jnp.float32)
    return mixed.astype(jnp.bfloat16)
```

```python
import math

import jax
import jax.numpy as jnp
import numpy as np
from jax import lax
from jax.experimental import pallas as pl
from jax.experimental.pallas import tpu as pltpu
from jax.sharding import PartitionSpec as P

HEADS = 32
KV_HEADS = 8
HEAD_SIZE = 128
LONGEST = 12288
DOCS = 6
TOK = 512
GROUP = 4
ROWS = GROUP * TOK
BLK = 2 * TOK + 16
PENALTY = -(2.0**100)
SCALE = math.log2(math.e) / math.sqrt(HEAD_SIZE)
QC = 256

epsilon = 1e-05
rope_base = 500000.0


WIDTH = 4096
PIECE = 512
N_TP = 8
CH = 4
CR = TOK // CH
MESH = pl.DeviceIdType.MESH


def tp_places():
    t = lax.axis_index("tp")
    plane = (t // 4) * 4
    y = t % 4
    up = plane + (y + 1) % 4
    down = plane + (y + 3) % 4
    far = plane + (y + 2) % 4
    return t, up, down, far


def other(t):
    return (t + 4) % 8


def greet(axis, peers):
    barrier = pltpu.get_barrier_semaphore()
    for peer in peers:
        pl.semaphore_signal(barrier, inc=1, device_id={axis: peer}, device_id_type=MESH)
    pl.semaphore_wait(barrier, len(peers))


def part(chunk):
    return pl.ds(chunk * CR, CR)


def project_kernel(
    h_ref, gain_ref, freq_ref, doc_ref, wq, wk, wv, q_out, kv_out,
    gath, w, acc, squares, cosine, sine, wsem, ssem, rsem, qssem, qrsem,
):
    t, up, down, far = tp_places()
    across = other(t)
    weights = [
        pltpu.make_async_copy(wq, w.at[:, 0:512], wsem.at[0]),
        pltpu.make_async_copy(wk, w.at[:, 512:640], wsem.at[1]),
        pltpu.make_async_copy(wv, w.at[:, 640:768], wsem.at[2]),
    ]
    for copy in weights:
        copy.start()
    peers = [(t + i) % N_TP for i in range(1, N_TP)]
    greet("tp", peers)
    sent = []

    def send(source, owner, chunk, to):
        copy = pltpu.make_async_remote_copy(
            src_ref=source,
            dst_ref=gath.at[owner, part(chunk)],
            send_sem=ssem.at[len(sent)],
            recv_sem=rsem.at[owner, chunk],
            device_id={"tp": to},
            device_id_type=MESH,
        )
        copy.start()
        sent.append(copy)

    def arrived(owner, chunk):
        pltpu.make_async_remote_copy(
            src_ref=gath.at[owner, part(chunk)],
            dst_ref=gath.at[owner, part(chunk)],
            send_sem=ssem.at[0],
            recv_sem=rsem.at[owner, chunk],
            device_id={"tp": across},
            device_id_type=MESH,
        ).wait_recv()

    upward = (0, 1, 2, 3)
    downward = (2, 3, 0, 1)

    def send_own(i):
        send(h_ref.at[part(upward[i])], t, upward[i], up)
        send(h_ref.at[part(downward[i])], t, downward[i], down)
        send(h_ref.at[part(upward[i])], t, upward[i], across)

    send_own(0)
    mine = h_ref[...].astype(jnp.float32)
    mass = jnp.sum(mine * mine, axis=1, keepdims=True)
    squares[t] = jnp.broadcast_to(mass, (TOK, 128)).T[0:8]
    told = []
    for i, peer in enumerate(peers):
        copy = pltpu.make_async_remote_copy(
            src_ref=squares.at[t],
            dst_ref=squares.at[t],
            send_sem=qssem.at[i],
            recv_sem=qrsem.at[t],
            device_id={"tp": peer},
            device_id_type=MESH,
        )
        copy.start()
        told.append(copy)
    for i in range(1, CH):
        send_own(i)

    first = lax.axis_index("cp") * TOK
    place = (first + lax.broadcasted_iota(jnp.int32, (HEAD_SIZE // 2, TOK), 1)).astype(jnp.float32)
    angle = place * freq_ref[...]
    cosine[...] = jnp.cos(angle)
    sine[...] = jnp.sin(angle)
    for peer in peers:
        pltpu.make_async_remote_copy(
            src_ref=squares.at[peer],
            dst_ref=squares.at[peer],
            send_sem=qssem.at[0],
            recv_sem=qrsem.at[peer],
            device_id={"tp": peer},
            device_id_type=MESH,
        ).wait_recv()
    whole = jnp.sum(squares[...], axis=0)[0:1]
    inverse = lax.rsqrt(whole / WIDTH + epsilon)
    inverse = jnp.broadcast_to(inverse, (128, TOK)).T
    inverse = jnp.concatenate([inverse] * (PIECE // 128), axis=1)
    for copy in weights:
        copy.wait()

    def use(source, owner, start):
        gain = gain_ref[pl.ds(owner, 1), :]
        normed = (source[...].astype(jnp.float32) * inverse * gain).astype(jnp.bfloat16)
        rows = pl.ds(pl.multiple_of(owner * PIECE, PIECE), PIECE)
        product = jnp.dot(normed, w[rows, :], preferred_element_type=jnp.float32)
        if start:
            acc[...] = product
        else:
            acc[...] += product

    use(h_ref, t, True)
    for i in range(CH):
        arrived(down, upward[i])
        if i < 2:
            send(gath.at[down, part(upward[i])], down, upward[i], up)
        arrived(up, downward[i])
        if i < 2:
            send(gath.at[up, part(downward[i])], up, downward[i], down)
        arrived(across, upward[i])
        if i == 1:
            for chunk in (0, 1):
                send(gath.at[across, part(chunk)], across, chunk, up)
                send(gath.at[across, part(chunk)], across, chunk, down)
        if i > 1:
            send(gath.at[across, part(i)], across, i, up)
            send(gath.at[across, part(i)], across, i, down)
    use(gath.at[up], up, False)
    use(gath.at[down], down, False)
    for i in range(2):
        for chunk in (upward[i], downward[i]):
            arrived(far, chunk)
            send(gath.at[far, part(chunk)], far, chunk, across)
    use(gath.at[across], across, False)
    use(gath.at[far], far, False)
    for chunk in (0, 2, 1, 3):
        arrived(other(far), chunk)
    use(gath.at[other(far)], other(far), False)
    for side in (up, down):
        for chunk in range(CH):
            arrived(other(side), chunk)
        use(gath.at[other(side)], other(side), False)

    half = HEAD_SIZE // 2
    for head in range(GROUP + 1):
        raw = acc[:, head * HEAD_SIZE : (head + 1) * HEAD_SIZE].T
        a = raw[:half]
        b = raw[half:]
        low = a * cosine[...] - b * sine[...]
        high = b * cosine[...] + a * sine[...]
        if head < GROUP:
            cols = slice(head * TOK, (head + 1) * TOK)
            q_out[0:half, cols] = low.astype(jnp.bfloat16)
            q_out[half:, cols] = high.astype(jnp.bfloat16)
        else:
            turned = jnp.concatenate([low, high], axis=0).T
            kv_out[0:TOK, :] = turned.astype(jnp.bfloat16)
    value = acc[:, (GROUP + 1) * HEAD_SIZE :].T.astype(jnp.bfloat16)
    for i in range(TOK // 128):
        kv_out[TOK + 128 * i : TOK + 128 * (i + 1), :] = value[:, 128 * i : 128 * (i + 1)]
    lane = lax.broadcasted_iota(jnp.int32, (16, 128), 1)
    row = lax.broadcasted_iota(jnp.int32, (16, 128), 0)
    tail = jnp.zeros((16, 128), jnp.int32)
    for d in range(1, DOCS):
        count = jnp.sum(jnp.where(doc_ref[...] < d, 1, 0), axis=1, keepdims=True)
        tail = jnp.where(
            (lane == d) & (row == 0), count // 16, jnp.where((lane == d) & (row == 1), count % 16, tail)
        )
    kv_out[2 * TOK :, :] = tail.astype(jnp.float32).astype(jnp.bfloat16)
    for copy in sent + told:
        copy.wait_send()


def project(hidden, norm_gain, w_query, w_key, w_value, doc_ids):
    vmem = pl.BlockSpec(memory_space=pltpu.VMEM)
    hbm = pl.BlockSpec(memory_space=pl.ANY)
    powers = -np.arange(HEAD_SIZE // 2, dtype=np.float32) * np.float32(2.0) / HEAD_SIZE
    freqs = (np.float64(rope_base) ** powers.astype(np.float64)).astype(np.float32)
    freqs = jnp.asarray(np.broadcast_to(freqs[:, None], (HEAD_SIZE // 2, TOK)))
    return pl.pallas_call(
        project_kernel,
        out_shape=(
            jax.ShapeDtypeStruct((HEAD_SIZE, ROWS), jnp.bfloat16),
            jax.ShapeDtypeStruct((BLK, 128), jnp.bfloat16),
        ),
        in_specs=[vmem] * 4 + [hbm] * 3,
        out_specs=(vmem, vmem),
        scratch_shapes=[
            pltpu.VMEM((N_TP, TOK, PIECE), jnp.bfloat16),
            pltpu.VMEM((WIDTH, 768), jnp.bfloat16),
            pltpu.VMEM((TOK, 768), jnp.float32),
            pltpu.VMEM((N_TP, 8, TOK), jnp.float32),
            pltpu.VMEM((HEAD_SIZE // 2, TOK), jnp.float32),
            pltpu.VMEM((HEAD_SIZE // 2, TOK), jnp.float32),
            pltpu.SemaphoreType.DMA((3,)),
            pltpu.SemaphoreType.DMA((28,)),
            pltpu.SemaphoreType.DMA((N_TP, CH)),
            pltpu.SemaphoreType.DMA((N_TP - 1,)),
            pltpu.SemaphoreType.DMA((N_TP,)),
        ],
        compiler_params=pltpu.CompilerParams(
            collective_id=0, has_side_effects=True, vmem_limit_bytes=48 * 2**20
        ),
        name="project",
    )(hidden, norm_gain.reshape(N_TP, PIECE), freqs, doc_ids, w_query, w_key, w_value)


def combine_kernel(
    att, w_out, out_ref,
    w, terms, sums, across_in, side_in, half_in, side_end, across_end,
    wsem, ssem, rsem,
):
    t, up, down, far = tp_places()
    across = other(t)
    order = [other(far), other(up), other(down), far, across, up, down, t]
    weights = []
    for i, owner in enumerate(order):
        cols = pl.ds(pl.multiple_of(owner * PIECE, PIECE), PIECE)
        weights.append(pltpu.make_async_copy(w_out.at[:, cols], w.at[i], wsem.at[i]))
        weights[-1].start()
    greet("tp", (up, down, across))
    sent = []

    def send(source, target, number, to):
        copy = pltpu.make_async_remote_copy(
            src_ref=source,
            dst_ref=target,
            send_sem=ssem.at[len(sent)],
            recv_sem=rsem.at[number],
            device_id={"tp": to},
            device_id_type=MESH,
        )
        copy.start()
        sent.append(copy)

    def arrived(target, number):
        pltpu.make_async_remote_copy(
            src_ref=target,
            dst_ref=target,
            send_sem=ssem.at[0],
            recv_sem=rsem.at[number],
            device_id={"tp": across},
            device_id_type=MESH,
        ).wait_recv()
        return target[...].astype(jnp.float32)

    def compute(i):
        weights[i].wait()
        product = jnp.dot(att[...], w[i], preferred_element_type=jnp.float32)
        terms[i] = product.astype(jnp.bfloat16)

    def term(i, chunk):
        return terms[i, part(chunk)].astype(jnp.float32)

    UP, DOWN = 0, 1
    compute(0)
    for chunk in (0, 2, 1, 3):
        send(terms.at[0, part(chunk)], across_in.at[part(chunk)], chunk, across)
    compute(1)
    compute(2)
    for chunk in range(CH):
        send(terms.at[1, part(chunk)], side_in.at[DOWN, part(chunk)], 4 + chunk, up)
        send(terms.at[2, part(chunk)], side_in.at[UP, part(chunk)], 8 + chunk, down)
    for i in range(3, 8):
        compute(i)
    for chunk in (0, 2, 1, 3):
        got = arrived(across_in.at[part(chunk)], chunk)
        sums[0, part(chunk)] = (term(3, chunk) + got).astype(jnp.bfloat16)
        if chunk < 2:
            send(sums.at[0, part(chunk)], half_in.at[DOWN, part(chunk)], 12 + chunk, up)
        else:
            send(sums.at[0, part(chunk)], half_in.at[UP, part(chunk - 2)], 12 + chunk, down)
    for chunk in range(CH):
        below = arrived(side_in.at[DOWN, part(chunk)], 4 + chunk)
        above = arrived(side_in.at[UP, part(chunk)], 8 + chunk)
        sums[1, part(chunk)] = (term(4, chunk) + below + above).astype(jnp.bfloat16)
        send(sums.at[1, part(chunk)], across_end.at[part(chunk)], 16 + chunk, across)
    for i in range(2):
        send(terms.at[5, part(2 + i)], side_end.at[DOWN, part(2 + i)], 22 + i, up)
        send(terms.at[6, part(i)], side_end.at[UP, part(i)], 24 + i, down)
    for i in range(2):
        got = arrived(half_in.at[DOWN, part(i)], 12 + i)
        sums[2, part(i)] = (term(5, i) + got).astype(jnp.bfloat16)
        send(sums.at[2, part(i)], side_end.at[DOWN, part(i)], 20 + i, up)
        got = arrived(half_in.at[UP, part(i)], 14 + i)
        sums[3, part(2 + i)] = (term(6, 2 + i) + got).astype(jnp.bfloat16)
        send(sums.at[3, part(2 + i)], side_end.at[UP, part(2 + i)], 26 + i, down)
    for chunk in range(CH):
        total = term(7, chunk) + arrived(across_end.at[part(chunk)], 16 + chunk)
        total = total + arrived(side_end.at[DOWN, part(chunk)], 20 + chunk)
        total = total + arrived(side_end.at[UP, part(chunk)], 24 + chunk)
        out_ref[part(chunk), :] = total.astype(jnp.bfloat16)
    for copy in sent:
        copy.wait_send()


def combine(attended, w_out):
    vmem = pl.BlockSpec(memory_space=pltpu.VMEM)
    hbm = pl.BlockSpec(memory_space=pl.ANY)
    return pl.pallas_call(
        combine_kernel,
        out_shape=jax.ShapeDtypeStruct((TOK, PIECE), jnp.bfloat16),
        in_specs=[vmem, hbm],
        out_specs=vmem,
        scratch_shapes=[
            pltpu.VMEM((N_TP, PIECE, PIECE), jnp.bfloat16),
            pltpu.VMEM((N_TP, TOK, PIECE), jnp.bfloat16),
            pltpu.VMEM((4, TOK, PIECE), jnp.bfloat16),
            pltpu.VMEM((TOK, PIECE), jnp.bfloat16),
            pltpu.VMEM((2, TOK, PIECE), jnp.bfloat16),
            pltpu.VMEM((2, TOK // 2, PIECE), jnp.bfloat16),
            pltpu.VMEM((2, TOK, PIECE), jnp.bfloat16),
            pltpu.VMEM((TOK, PIECE), jnp.bfloat16),
            pltpu.SemaphoreType.DMA((N_TP,)),
            pltpu.SemaphoreType.DMA((28,)),
            pltpu.SemaphoreType.DMA((28,)),
        ],
        compiler_params=pltpu.CompilerParams(
            collective_id=1, has_side_effects=True, vmem_limit_bytes=40 * 2**20
        ),
        name="combine",
    )(attended, w_out)


def augment_queries(q_ref, doc_ref, qaug):
    qaug[0:HEAD_SIZE, :] = q_ref[...]
    row = lax.broadcasted_iota(jnp.int32, (HEAD_SIZE, TOK), 0)
    hot = jnp.where(row == doc_ref[...], PENALTY, 0.0).astype(jnp.bfloat16)
    for head in range(GROUP):
        qaug[HEAD_SIZE:, head * TOK : (head + 1) * TOK] = hot


def attend(block, qaug, best, total, acc, first):
    keys = block[0:TOK, :]
    counts = block[2 * TOK : 2 * TOK + 2, :].astype(jnp.float32)
    below = counts[0:1] * 16.0 + counts[1:2]
    row = lax.broadcasted_iota(jnp.int32, (TOK, HEAD_SIZE), 0).astype(jnp.float32)
    earlier = jnp.where(row < below, 1.0, 0.0).astype(jnp.bfloat16)
    keys = jnp.concatenate([keys, earlier], axis=1)
    values = jnp.concatenate(
        [block[TOK + 128 * i : TOK + 128 * (i + 1), :] for i in range(TOK // 128)], axis=1
    )
    for chunk in range(ROWS // QC):
        cols = slice(chunk * QC, (chunk + 1) * QC)
        scores = jnp.dot(keys, qaug[:, cols], preferred_element_type=jnp.float32)
        if first:
            key_at = lax.broadcasted_iota(jnp.int32, (TOK, QC), 0)
            query_at = lax.broadcasted_iota(jnp.int32, (TOK, QC), 1) + (chunk * QC) % TOK
            scores = jnp.where(key_at <= query_at, scores, jnp.float32(PENALTY))
            top = jnp.max(scores, axis=0, keepdims=True)
        else:
            old = best[:, cols]
            top = jnp.maximum(old, jnp.max(scores, axis=0, keepdims=True))
        weights = jnp.exp2(scores * SCALE - top * SCALE)
        mass = jnp.sum(weights, axis=0, keepdims=True)
        out = jnp.dot(values, weights.astype(jnp.bfloat16), preferred_element_type=jnp.float32)
        if first:
            total[:, cols] = mass
            acc[:, cols] = out
        else:
            shrink = jnp.exp2((old - top) * SCALE)
            total[:, cols] = total[:, cols] * shrink + mass
            acc[:, cols] = acc[:, cols] * shrink + out
        best[:, cols] = top


def finish(total, acc, out_ref):
    for head in range(GROUP):
        cols = slice(head * TOK, (head + 1) * TOK)
        out_ref[:, head * HEAD_SIZE : (head + 1) * HEAD_SIZE] = (
            (acc[:, cols] / total[:, cols]).T.astype(jnp.bfloat16)
        )


def attention_kernel(q_ref, doc_ref, kv_ref, out_ref, qaug, best, total, acc):
    me = lax.axis_index("cp")
    augment_queries(q_ref, doc_ref, qaug)
    attend(kv_ref.at[me], qaug, best, total, acc, True)

    @pl.loop(jnp.maximum(me - LONGEST // TOK, 0), me)
    def _(j):
        attend(kv_ref.at[j], qaug, best, total, acc, False)

    finish(total, acc, out_ref)


def attention(queries, docs, blocks):
    vmem = pl.BlockSpec(memory_space=pltpu.VMEM)
    return pl.pallas_call(
        attention_kernel,
        out_shape=jax.ShapeDtypeStruct((TOK, GROUP * HEAD_SIZE), jnp.bfloat16),
        in_specs=[vmem] * 3,
        out_specs=vmem,
        scratch_shapes=[
            pltpu.VMEM((2 * HEAD_SIZE, ROWS), jnp.bfloat16),
            pltpu.VMEM((1, ROWS), jnp.float32),
            pltpu.VMEM((1, ROWS), jnp.float32),
            pltpu.VMEM((HEAD_SIZE, ROWS), jnp.float32),
        ],
        compiler_params=pltpu.CompilerParams(vmem_limit_bytes=40 * 2**20),
        name="attention",
    )(queries, docs, blocks)


def shards(hidden, norm_gain, w_query, w_key, w_value, w_out, doc_ids):
    docs = doc_ids.reshape(1, TOK)
    queries, block = project(hidden, norm_gain, w_query, w_key, w_value, docs)
    blocks = lax.all_gather(block, "cp", axis=0, tiled=False)
    attended = attention(queries, docs, blocks)
    return combine(attended, w_out)


def solution(mesh):
    in_specs = (
        P("cp", "tp"),
        P(),
        P(None, "tp"),
        P(None, "tp"),
        P(None, "tp"),
        P("tp", None),
        P("cp"),
    )
    return jax.shard_map(
        shards, mesh=mesh, in_specs=in_specs, out_specs=P("cp", "tp"), check_vma=False
    )
```

```python
import math

import jax
import jax.numpy as jnp
import numpy as np
from jax import lax
from jax.experimental import pallas as pl
from jax.experimental.pallas import tpu as pltpu
from jax.sharding import PartitionSpec as P

HEADS = 32
KV_HEADS = 8
HEAD_SIZE = 128
LONGEST = 12288
DOCS = 6
TOK = 512
GROUP = 4
ROWS = GROUP * TOK
BLK = 2 * TOK + 16
PENALTY = -(2.0**100)
SCALE = math.log2(math.e) / math.sqrt(HEAD_SIZE)
QC = 512

epsilon = 1e-05
rope_base = 500000.0


WIDTH = 4096
PIECE = 512
N_TP = 8
CH = 4
CR = TOK // CH
MESH = pl.DeviceIdType.MESH


def tp_places():
    t = lax.axis_index("tp")
    plane = (t // 4) * 4
    y = t % 4
    up = plane + (y + 1) % 4
    down = plane + (y + 3) % 4
    far = plane + (y + 2) % 4
    return t, up, down, far


def other(t):
    return (t + 4) % 8


def greet(axis, peers):
    barrier = pltpu.get_barrier_semaphore()
    for peer in peers:
        pl.semaphore_signal(barrier, inc=1, device_id={axis: peer}, device_id_type=MESH)
    pl.semaphore_wait(barrier, len(peers))


def part(chunk):
    return pl.ds(chunk * CR, CR)


def project_kernel(
    h_ref, gain_ref, freq_ref, doc_ref, wq, wk, wv, q_out, kv_out,
    gath, w, acc, squares, cosine, sine, wsem, ssem, rsem, qssem, qrsem,
):
    t, up, down, far = tp_places()
    across = other(t)
    weights = [
        pltpu.make_async_copy(wq, w.at[:, 0:512], wsem.at[0]),
        pltpu.make_async_copy(wk, w.at[:, 512:640], wsem.at[1]),
        pltpu.make_async_copy(wv, w.at[:, 640:768], wsem.at[2]),
    ]
    for copy in weights:
        copy.start()
    peers = [(t + i) % N_TP for i in range(1, N_TP)]
    greet("tp", peers)
    sent = []

    def send(source, owner, chunk, to):
        copy = pltpu.make_async_remote_copy(
            src_ref=source,
            dst_ref=gath.at[owner, part(chunk)],
            send_sem=ssem.at[len(sent)],
            recv_sem=rsem.at[owner, chunk],
            device_id={"tp": to},
            device_id_type=MESH,
        )
        copy.start()
        sent.append(copy)

    def arrived(owner, chunk):
        pltpu.make_async_remote_copy(
            src_ref=gath.at[owner, part(chunk)],
            dst_ref=gath.at[owner, part(chunk)],
            send_sem=ssem.at[0],
            recv_sem=rsem.at[owner, chunk],
            device_id={"tp": across},
            device_id_type=MESH,
        ).wait_recv()

    upward = (0, 1, 2, 3)
    downward = (2, 3, 0, 1)

    def send_own(i):
        send(h_ref.at[part(upward[i])], t, upward[i], up)
        send(h_ref.at[part(downward[i])], t, downward[i], down)
        send(h_ref.at[part(upward[i])], t, upward[i], across)

    send_own(0)
    mine = h_ref[...].astype(jnp.float32)
    mass = jnp.sum(mine * mine, axis=1, keepdims=True)
    squares[t] = jnp.broadcast_to(mass, (TOK, 128)).T[0:8]
    told = []
    for i, peer in enumerate(peers):
        copy = pltpu.make_async_remote_copy(
            src_ref=squares.at[t],
            dst_ref=squares.at[t],
            send_sem=qssem.at[i],
            recv_sem=qrsem.at[t],
            device_id={"tp": peer},
            device_id_type=MESH,
        )
        copy.start()
        told.append(copy)
    for i in range(1, CH):
        send_own(i)

    first = lax.axis_index("cp") * TOK
    place = (first + lax.broadcasted_iota(jnp.int32, (HEAD_SIZE // 2, TOK), 1)).astype(jnp.float32)
    angle = place * freq_ref[...]
    cosine[...] = jnp.cos(angle)
    sine[...] = jnp.sin(angle)
    for peer in peers:
        pltpu.make_async_remote_copy(
            src_ref=squares.at[peer],
            dst_ref=squares.at[peer],
            send_sem=qssem.at[0],
            recv_sem=qrsem.at[peer],
            device_id={"tp": peer},
            device_id_type=MESH,
        ).wait_recv()
    whole = jnp.sum(squares[...], axis=0)[0:1]
    inverse = lax.rsqrt(whole / WIDTH + epsilon)
    inverse = jnp.broadcast_to(inverse, (128, TOK)).T
    inverse = jnp.concatenate([inverse] * (PIECE // 128), axis=1)
    for copy in weights:
        copy.wait()

    def use(source, owner, start):
        gain = gain_ref[pl.ds(owner, 1), :]
        normed = (source[...].astype(jnp.float32) * inverse * gain).astype(jnp.bfloat16)
        rows = pl.ds(pl.multiple_of(owner * PIECE, PIECE), PIECE)
        product = jnp.dot(normed, w[rows, :], preferred_element_type=jnp.float32)
        if start:
            acc[...] = product
        else:
            acc[...] += product

    use(h_ref, t, True)
    for i in range(CH):
        arrived(down, upward[i])
        if i < 2:
            send(gath.at[down, part(upward[i])], down, upward[i], up)
        arrived(up, downward[i])
        if i < 2:
            send(gath.at[up, part(downward[i])], up, downward[i], down)
        arrived(across, upward[i])
        if i == 1:
            for chunk in (0, 1):
                send(gath.at[across, part(chunk)], across, chunk, up)
                send(gath.at[across, part(chunk)], across, chunk, down)
        if i > 1:
            send(gath.at[across, part(i)], across, i, up)
            send(gath.at[across, part(i)], across, i, down)
    use(gath.at[up], up, False)
    use(gath.at[down], down, False)
    for i in range(2):
        for chunk in (upward[i], downward[i]):
            arrived(far, chunk)
            send(gath.at[far, part(chunk)], far, chunk, across)
    use(gath.at[across], across, False)
    use(gath.at[far], far, False)
    for chunk in (0, 2, 1, 3):
        arrived(other(far), chunk)
    use(gath.at[other(far)], other(far), False)
    for side in (up, down):
        for chunk in range(CH):
            arrived(other(side), chunk)
        use(gath.at[other(side)], other(side), False)

    half = HEAD_SIZE // 2
    for head in range(GROUP + 1):
        raw = acc[:, head * HEAD_SIZE : (head + 1) * HEAD_SIZE].T
        a = raw[:half]
        b = raw[half:]
        low = a * cosine[...] - b * sine[...]
        high = b * cosine[...] + a * sine[...]
        if head < GROUP:
            cols = slice(head * TOK, (head + 1) * TOK)
            q_out[0:half, cols] = low.astype(jnp.bfloat16)
            q_out[half:, cols] = high.astype(jnp.bfloat16)
        else:
            turned = jnp.concatenate([low, high], axis=0).T
            kv_out[0:TOK, :] = turned.astype(jnp.bfloat16)
    value = acc[:, (GROUP + 1) * HEAD_SIZE :].T.astype(jnp.bfloat16)
    for i in range(TOK // 128):
        kv_out[TOK + 128 * i : TOK + 128 * (i + 1), :] = value[:, 128 * i : 128 * (i + 1)]
    lane = lax.broadcasted_iota(jnp.int32, (16, 128), 1)
    row = lax.broadcasted_iota(jnp.int32, (16, 128), 0)
    tail = jnp.zeros((16, 128), jnp.int32)
    for d in range(1, DOCS):
        count = jnp.sum(jnp.where(doc_ref[...] < d, 1, 0), axis=1, keepdims=True)
        tail = jnp.where(
            (lane == d) & (row == 0), count // 16, jnp.where((lane == d) & (row == 1), count % 16, tail)
        )
    kv_out[2 * TOK :, :] = tail.astype(jnp.float32).astype(jnp.bfloat16)
    for copy in sent + told:
        copy.wait_send()


def project(hidden, norm_gain, w_query, w_key, w_value, doc_ids):
    vmem = pl.BlockSpec(memory_space=pltpu.VMEM)
    hbm = pl.BlockSpec(memory_space=pl.ANY)
    powers = -np.arange(HEAD_SIZE // 2, dtype=np.float32) * np.float32(2.0) / HEAD_SIZE
    freqs = (np.float64(rope_base) ** powers.astype(np.float64)).astype(np.float32)
    freqs = jnp.asarray(np.broadcast_to(freqs[:, None], (HEAD_SIZE // 2, TOK)))
    return pl.pallas_call(
        project_kernel,
        out_shape=(
            jax.ShapeDtypeStruct((HEAD_SIZE, ROWS), jnp.bfloat16),
            jax.ShapeDtypeStruct((BLK, 128), jnp.bfloat16),
        ),
        in_specs=[vmem] * 4 + [hbm] * 3,
        out_specs=(vmem, vmem),
        scratch_shapes=[
            pltpu.VMEM((N_TP, TOK, PIECE), jnp.bfloat16),
            pltpu.VMEM((WIDTH, 768), jnp.bfloat16),
            pltpu.VMEM((TOK, 768), jnp.float32),
            pltpu.VMEM((N_TP, 8, TOK), jnp.float32),
            pltpu.VMEM((HEAD_SIZE // 2, TOK), jnp.float32),
            pltpu.VMEM((HEAD_SIZE // 2, TOK), jnp.float32),
            pltpu.SemaphoreType.DMA((3,)),
            pltpu.SemaphoreType.DMA((28,)),
            pltpu.SemaphoreType.DMA((N_TP, CH)),
            pltpu.SemaphoreType.DMA((N_TP - 1,)),
            pltpu.SemaphoreType.DMA((N_TP,)),
        ],
        compiler_params=pltpu.CompilerParams(
            collective_id=0, has_side_effects=True, vmem_limit_bytes=48 * 2**20
        ),
        name="project",
    )(hidden, norm_gain.reshape(N_TP, PIECE), freqs, doc_ids, w_query, w_key, w_value)


def combine_kernel(
    att, w_out, out_ref,
    w, terms, sums, across_in, side_in, half_in, side_end, across_end,
    wsem, ssem, rsem,
):
    t, up, down, far = tp_places()
    across = other(t)
    order = [other(far), other(up), other(down), far, across, up, down, t]
    weights = []
    for i, owner in enumerate(order):
        cols = pl.ds(pl.multiple_of(owner * PIECE, PIECE), PIECE)
        weights.append(pltpu.make_async_copy(w_out.at[:, cols], w.at[i], wsem.at[i]))
        weights[-1].start()
    greet("tp", (up, down, across))
    sent = []

    def send(source, target, number, to):
        copy = pltpu.make_async_remote_copy(
            src_ref=source,
            dst_ref=target,
            send_sem=ssem.at[len(sent)],
            recv_sem=rsem.at[number],
            device_id={"tp": to},
            device_id_type=MESH,
        )
        copy.start()
        sent.append(copy)

    def arrived(target, number):
        pltpu.make_async_remote_copy(
            src_ref=target,
            dst_ref=target,
            send_sem=ssem.at[0],
            recv_sem=rsem.at[number],
            device_id={"tp": across},
            device_id_type=MESH,
        ).wait_recv()
        return target[...].astype(jnp.float32)

    def compute(i):
        weights[i].wait()
        product = jnp.dot(att[...], w[i], preferred_element_type=jnp.float32)
        terms[i] = product.astype(jnp.bfloat16)

    def term(i, chunk):
        return terms[i, part(chunk)].astype(jnp.float32)

    UP, DOWN = 0, 1
    compute(0)
    for chunk in (0, 2, 1, 3):
        send(terms.at[0, part(chunk)], across_in.at[part(chunk)], chunk, across)
    compute(1)
    compute(2)
    for chunk in range(CH):
        send(terms.at[1, part(chunk)], side_in.at[DOWN, part(chunk)], 4 + chunk, up)
        send(terms.at[2, part(chunk)], side_in.at[UP, part(chunk)], 8 + chunk, down)
    for i in range(3, 8):
        compute(i)
    for chunk in (0, 2, 1, 3):
        got = arrived(across_in.at[part(chunk)], chunk)
        sums[0, part(chunk)] = (term(3, chunk) + got).astype(jnp.bfloat16)
        if chunk < 2:
            send(sums.at[0, part(chunk)], half_in.at[DOWN, part(chunk)], 12 + chunk, up)
        else:
            send(sums.at[0, part(chunk)], half_in.at[UP, part(chunk - 2)], 12 + chunk, down)
    for chunk in range(CH):
        below = arrived(side_in.at[DOWN, part(chunk)], 4 + chunk)
        above = arrived(side_in.at[UP, part(chunk)], 8 + chunk)
        sums[1, part(chunk)] = (term(4, chunk) + below + above).astype(jnp.bfloat16)
        send(sums.at[1, part(chunk)], across_end.at[part(chunk)], 16 + chunk, across)
    for i in range(2):
        send(terms.at[5, part(2 + i)], side_end.at[DOWN, part(2 + i)], 22 + i, up)
        send(terms.at[6, part(i)], side_end.at[UP, part(i)], 24 + i, down)
    for i in range(2):
        got = arrived(half_in.at[DOWN, part(i)], 12 + i)
        sums[2, part(i)] = (term(5, i) + got).astype(jnp.bfloat16)
        send(sums.at[2, part(i)], side_end.at[DOWN, part(i)], 20 + i, up)
        got = arrived(half_in.at[UP, part(i)], 14 + i)
        sums[3, part(2 + i)] = (term(6, 2 + i) + got).astype(jnp.bfloat16)
        send(sums.at[3, part(2 + i)], side_end.at[UP, part(2 + i)], 26 + i, down)
    for chunk in range(CH):
        total = term(7, chunk) + arrived(across_end.at[part(chunk)], 16 + chunk)
        total = total + arrived(side_end.at[DOWN, part(chunk)], 20 + chunk)
        total = total + arrived(side_end.at[UP, part(chunk)], 24 + chunk)
        out_ref[part(chunk), :] = total.astype(jnp.bfloat16)
    for copy in sent:
        copy.wait_send()


def combine(attended, w_out):
    vmem = pl.BlockSpec(memory_space=pltpu.VMEM)
    hbm = pl.BlockSpec(memory_space=pl.ANY)
    return pl.pallas_call(
        combine_kernel,
        out_shape=jax.ShapeDtypeStruct((TOK, PIECE), jnp.bfloat16),
        in_specs=[vmem, hbm],
        out_specs=vmem,
        scratch_shapes=[
            pltpu.VMEM((N_TP, PIECE, PIECE), jnp.bfloat16),
            pltpu.VMEM((N_TP, TOK, PIECE), jnp.bfloat16),
            pltpu.VMEM((4, TOK, PIECE), jnp.bfloat16),
            pltpu.VMEM((TOK, PIECE), jnp.bfloat16),
            pltpu.VMEM((2, TOK, PIECE), jnp.bfloat16),
            pltpu.VMEM((2, TOK // 2, PIECE), jnp.bfloat16),
            pltpu.VMEM((2, TOK, PIECE), jnp.bfloat16),
            pltpu.VMEM((TOK, PIECE), jnp.bfloat16),
            pltpu.SemaphoreType.DMA((N_TP,)),
            pltpu.SemaphoreType.DMA((28,)),
            pltpu.SemaphoreType.DMA((28,)),
        ],
        compiler_params=pltpu.CompilerParams(
            collective_id=1, has_side_effects=True, vmem_limit_bytes=40 * 2**20
        ),
        name="combine",
    )(attended, w_out)


def augment_queries(q_ref, doc_ref, qaug):
    qaug[0:HEAD_SIZE, :] = q_ref[...]
    row = lax.broadcasted_iota(jnp.int32, (HEAD_SIZE, TOK), 0)
    hot = jnp.where(row == doc_ref[...], PENALTY, 0.0).astype(jnp.bfloat16)
    for head in range(GROUP):
        qaug[HEAD_SIZE:, head * TOK : (head + 1) * TOK] = hot


def attend_keys(block):
    counts = block[2 * TOK : 2 * TOK + 2, :].astype(jnp.float32)
    below = counts[0:1] * 16.0 + counts[1:2]
    row = lax.broadcasted_iota(jnp.int32, (TOK, HEAD_SIZE), 0).astype(jnp.float32)
    earlier = jnp.where(row < below, 1.0, 0.0).astype(jnp.bfloat16)
    return jnp.concatenate([block[0:TOK, :], earlier], axis=1)


def score(keys, chunk, qaug, logits, tops, causal):
    cols = slice(chunk * QC, (chunk + 1) * QC)
    scores = jnp.dot(keys, qaug[:, cols], preferred_element_type=jnp.float32)
    if causal:
        key_at = lax.broadcasted_iota(jnp.int32, (TOK, QC), 0)
        query_at = lax.broadcasted_iota(jnp.int32, (TOK, QC), 1) + (chunk * QC) % TOK
        scores = jnp.where(key_at <= query_at, scores, jnp.float32(PENALTY))
    logits[chunk % 2] = scores
    tops[chunk % 2] = jnp.max(scores, axis=0, keepdims=True)


def weigh(values, chunk, logits, tops, best, total, acc, first):
    cols = slice(chunk * QC, (chunk + 1) * QC)
    top = tops[chunk % 2]
    if not first:
        old = best[:, cols]
        top = jnp.maximum(old, top)
    weights = jnp.exp2(logits[chunk % 2] * SCALE - top * SCALE)
    mass = jnp.sum(weights, axis=0, keepdims=True)
    out = jnp.dot(values, weights.astype(jnp.bfloat16), preferred_element_type=jnp.float32)
    if first:
        total[:, cols] = mass
        acc[:, cols] = out
    else:
        shrink = jnp.exp2((old - top) * SCALE)
        total[:, cols] = total[:, cols] * shrink + mass
        acc[:, cols] = acc[:, cols] * shrink + out
    best[:, cols] = top


def attend(blocks, state, first):
    qaug, logits, tops, best, total, acc = state
    chunks = ROWS // QC
    keys = [attend_keys(block) for block in blocks]
    values = [
        jnp.concatenate(
            [block[TOK + 128 * i : TOK + 128 * (i + 1), :] for i in range(TOK // 128)], axis=1
        )
        for block in blocks
    ]
    score(keys[0], 0, qaug, logits, tops, first)
    for step in range(len(blocks) * chunks):
        if step + 1 < len(blocks) * chunks:
            which, chunk = divmod(step + 1, chunks)
            score(keys[which], chunk, qaug, logits, tops, first)
        which, chunk = divmod(step, chunks)
        weigh(values[which], chunk, logits, tops, best, total, acc, first)


def finish(total, acc, out_ref):
    for head in range(GROUP):
        cols = slice(head * TOK, (head + 1) * TOK)
        out_ref[:, head * HEAD_SIZE : (head + 1) * HEAD_SIZE] = (
            (acc[:, cols] / total[:, cols]).T.astype(jnp.bfloat16)
        )


ROLES = 15
PARTS = ((0, TOK), (TOK, TOK + 16))


def attention_kernel(
    q_ref, doc_ref, own_ref, out_ref,
    kv, qaug, logits, tops, best, total, acc, ssem, rsem, sibsend, sibrecv,
):
    me = lax.axis_index("cp")
    core = me % 2
    x = (me // 2) % 4
    z = me // 8
    state = (qaug, logits, tops, best, total, acc)

    def at(zz, xx):
        return (zz * 4 + xx) * 2 + core

    right = at(z, (x + 1) % 4)
    left = at(z, (x + 3) % 4)
    ahead = at((z + 1) % 4, x)
    behind = at((z + 3) % 4, x)
    sibling = me + 1 - 2 * core
    greet("cp", (right, left, ahead, behind, sibling))

    def move(source, slot, half, to, send_sem, recv_sem):
        rows = pl.ds(*PARTS[half])
        return pltpu.make_async_remote_copy(
            src_ref=source.at[rows],
            dst_ref=kv.at[slot, rows],
            send_sem=send_sem,
            recv_sem=recv_sem,
            device_id={"cp": to},
            device_id_type=MESH,
        )

    always = z >= 0
    top = z == 3
    one, two = z >= 1, z >= 2
    xm, xp, x2 = (x + 3) % 4, (x + 1) % 4, (x + 2) % 4
    roles = [
        (x >= 1, z, xm),
        (x == 3, z, xp),
        (x >= 2, z, x2),
        (one, (z + 3) % 4, x),
        (top, 0 * z, x),
        (one, (z + 3) % 4, xm),
        (one, (z + 3) % 4, xp),
        (top & (x < 3), 0 * z, xp),
        (top & (x == 0), 0 * z, xm),
        (one, (z + 3) % 4, x2),
        (top & (x < 2), 0 * z, x2),
        (two, (z + 2) % 4, x),
        (two, (z + 2) % 4, xm),
        (two, (z + 2) % 4, xp),
        (two, (z + 2) % 4, x2),
    ]
    slots = [at(zz, xx) for _, zz, xx in roles]
    middle = (x == 1) | (x == 2)
    forwards = {
        0: [(middle, right, (0, 1))],
        3: [(z < 3, ahead, (0, 1)), (always, right, (0, 1)), (always, left, (1, 0))],
        4: [(x > 0, left, (0, 1)), (x == 3, right, (0, 1))],
        5: [(always, right, (0,))],
        6: [(always, left, (1,))],
        7: [(middle, left, (0, 1))],
        11: [(always, right, (0, 1)), (always, left, (1, 0))],
        12: [(always, right, (0,))],
        13: [(always, left, (1,))],
    }
    sends = []

    def plan(when, source, slot, half, to):
        number = len(sends)
        sends.append((when, source, slot, half, to))
        return number

    def issue(number):
        when, source, slot, half, to = sends[number]

        @pl.when(when)
        def _():
            move(source, slot, half, to, ssem.at[number], rsem.at[slot, half]).start()

    own = []
    for half in (0, 1):
        own.append(plan(z < 3, own_ref, me, half, ahead))
        own.append(plan(z == 0, own_ref, me, half, behind))
        own.append(plan(x < 3, own_ref, me, half, right))
        own.append(plan(x == 0, own_ref, me, half, left))
    relays = {}
    for role, targets in forwards.items():
        relays[role] = {0: [], 1: []}
        for when, to, halves in targets:
            for half in halves:
                number = plan(roles[role][0] & when, kv.at[slots[role]], slots[role], half, to)
                relays[role][half].append(number)

    for half in (0, 1):
        move(own_ref, me, half, sibling, sibsend.at[ROLES, half], sibrecv.at[ROLES, half]).start()
    for number in own:
        issue(number)
    augment_queries(q_ref, doc_ref, qaug)
    attend([own_ref], state, True)
    for half in (0, 1):
        move(own_ref, sibling, half, sibling, sibsend.at[ROLES, half], sibrecv.at[ROLES, half]).wait_recv()

    @pl.when(core == 1)
    def _():
        attend([kv.at[sibling]], state, False)

    def serve(role):
        slot = slots[role]
        for half in (0, 1):

            @pl.when(roles[role][0])
            def _():
                move(own_ref, slot, half, sibling, ssem.at[0], rsem.at[slot, half]).wait_recv()
                move(
                    kv.at[slot], slot, half, sibling, sibsend.at[role, half], sibrecv.at[role, half]
                ).start()

            for number in relays.get(role, {0: [], 1: []})[half]:
                issue(number)

    @pl.loop(0, ROLES)
    def _(step):
        there = step < 0
        slot = 0 * step
        for role in range(ROLES):

            @pl.when(step == role)
            def _():
                serve(role)

            there = there | ((step == role) & roles[role][0])
            slot = jnp.where(step == role, slots[role], slot)

        @pl.when(there)
        def _():
            twin = slot + 1 - 2 * core
            for half in (0, 1):
                move(own_ref, twin, half, sibling, sibsend.at[step, half], sibrecv.at[step, half]).wait_recv()
            attend([kv.at[slot], kv.at[twin]], state, False)

    finish(total, acc, out_ref)
    for number, (when, source, slot, half, to) in enumerate(sends):

        @pl.when(when)
        def _():
            move(source, slot, half, to, ssem.at[number], rsem.at[slot, half]).wait_send()

    for role in range(ROLES + 1):
        present, slot = (always, me) if role == ROLES else (roles[role][0], slots[role])
        for half in (0, 1):

            @pl.when(present)
            def _():
                move(
                    own_ref, slot, half, sibling, sibsend.at[role, half], sibrecv.at[role, half]
                ).wait_send()


SENDS = 30


def attention(queries, docs, block):
    vmem = pl.BlockSpec(memory_space=pltpu.VMEM)
    return pl.pallas_call(
        attention_kernel,
        out_shape=jax.ShapeDtypeStruct((TOK, GROUP * HEAD_SIZE), jnp.bfloat16),
        in_specs=[vmem] * 3,
        out_specs=vmem,
        scratch_shapes=[
            pltpu.VMEM((32, BLK, 128), jnp.bfloat16),
            pltpu.VMEM((2 * HEAD_SIZE, ROWS), jnp.bfloat16),
            pltpu.VMEM((2, TOK, QC), jnp.float32),
            pltpu.VMEM((2, 1, QC), jnp.float32),
            pltpu.VMEM((1, ROWS), jnp.float32),
            pltpu.VMEM((1, ROWS), jnp.float32),
            pltpu.VMEM((HEAD_SIZE, ROWS), jnp.float32),
            pltpu.SemaphoreType.DMA((SENDS,)),
            pltpu.SemaphoreType.DMA((32, 2)),
            pltpu.SemaphoreType.DMA((ROLES + 1, 2)),
            pltpu.SemaphoreType.DMA((ROLES + 1, 2)),
        ],
        compiler_params=pltpu.CompilerParams(
            collective_id=2, has_side_effects=True, vmem_limit_bytes=40 * 2**20
        ),
        name="attention",
    )(queries, docs, block)


def shards(hidden, norm_gain, w_query, w_key, w_value, w_out, doc_ids):
    docs = doc_ids.reshape(1, TOK)
    queries, block = project(hidden, norm_gain, w_query, w_key, w_value, docs)
    attended = attention(queries, docs, block)
    return combine(attended, w_out)


def solution(mesh):
    in_specs = (
        P("cp", "tp"),
        P(),
        P(None, "tp"),
        P(None, "tp"),
        P(None, "tp"),
        P("tp", None),
        P("cp"),
    )
    return jax.shard_map(
        shards, mesh=mesh, in_specs=in_specs, out_specs=P("cp", "tp"), check_vma=False
    )
```

```python
import math

import jax
import jax.numpy as jnp
import numpy as np
from jax import lax
from jax.experimental import pallas as pl
from jax.experimental.pallas import tpu as pltpu
from jax.sharding import PartitionSpec as P

HEADS = 32
KV_HEADS = 8
HEAD_SIZE = 128
LONGEST = 12288
DOCS = 6
TOK = 512
GROUP = 4
ROWS = GROUP * TOK
BLK = 2 * TOK + 16
PENALTY = -(2.0**100)
SCALE = math.log2(math.e) / math.sqrt(HEAD_SIZE)
QC = 512

epsilon = 1e-05
rope_base = 500000.0


WIDTH = 4096
PIECE = 512
N_TP = 8
CH = 4
CR = TOK // CH
MESH = pl.DeviceIdType.MESH


def tp_places():
    t = lax.axis_index("tp")
    plane = (t // 4) * 4
    y = t % 4
    up = plane + (y + 1) % 4
    down = plane + (y + 3) % 4
    far = plane + (y + 2) % 4
    return t, up, down, far


def other(t):
    return (t + 4) % 8


def greet(axis, peers):
    barrier = pltpu.get_barrier_semaphore()
    for peer in peers:
        pl.semaphore_signal(barrier, inc=1, device_id={axis: peer}, device_id_type=MESH)
    pl.semaphore_wait(barrier, len(peers))


def part(chunk):
    return pl.ds(chunk * CR, CR)


def project_kernel(
    h_ref, gain_ref, freq_ref, doc_ref, wq, wk, wv, q_out, kv_out,
    gath, w, acc, squares, cosine, sine, wsem, ssem, rsem, qssem, qrsem,
):
    t, up, down, far = tp_places()
    across = other(t)
    weights = [
        pltpu.make_async_copy(wq, w.at[:, 0:512], wsem.at[0]),
        pltpu.make_async_copy(wk, w.at[:, 512:640], wsem.at[1]),
        pltpu.make_async_copy(wv, w.at[:, 640:768], wsem.at[2]),
    ]
    for copy in weights:
        copy.start()
    peers = [(t + i) % N_TP for i in range(1, N_TP)]
    greet("tp", peers)
    sent = []

    def send(source, owner, chunk, to):
        copy = pltpu.make_async_remote_copy(
            src_ref=source,
            dst_ref=gath.at[owner, part(chunk)],
            send_sem=ssem.at[len(sent)],
            recv_sem=rsem.at[owner, chunk],
            device_id={"tp": to},
            device_id_type=MESH,
        )
        copy.start()
        sent.append(copy)

    def arrived(owner, chunk):
        pltpu.make_async_remote_copy(
            src_ref=gath.at[owner, part(chunk)],
            dst_ref=gath.at[owner, part(chunk)],
            send_sem=ssem.at[0],
            recv_sem=rsem.at[owner, chunk],
            device_id={"tp": across},
            device_id_type=MESH,
        ).wait_recv()

    upward = (0, 1, 2, 3)
    downward = (2, 3, 0, 1)

    def send_own(i):
        send(h_ref.at[part(upward[i])], t, upward[i], up)
        send(h_ref.at[part(downward[i])], t, downward[i], down)
        send(h_ref.at[part(upward[i])], t, upward[i], across)

    send_own(0)
    mine = h_ref[...].astype(jnp.float32)
    mass = jnp.sum(mine * mine, axis=1, keepdims=True)
    squares[t] = jnp.broadcast_to(mass, (TOK, 128)).T[0:8]
    told = []
    for i, peer in enumerate(peers):
        copy = pltpu.make_async_remote_copy(
            src_ref=squares.at[t],
            dst_ref=squares.at[t],
            send_sem=qssem.at[i],
            recv_sem=qrsem.at[t],
            device_id={"tp": peer},
            device_id_type=MESH,
        )
        copy.start()
        told.append(copy)
    for i in range(1, CH):
        send_own(i)

    first = lax.axis_index("cp") * TOK
    place = (first + lax.broadcasted_iota(jnp.int32, (HEAD_SIZE // 2, TOK), 1)).astype(jnp.float32)
    angle = place * freq_ref[...]
    cosine[...] = jnp.cos(angle)
    sine[...] = jnp.sin(angle)
    for peer in peers:
        pltpu.make_async_remote_copy(
            src_ref=squares.at[peer],
            dst_ref=squares.at[peer],
            send_sem=qssem.at[0],
            recv_sem=qrsem.at[peer],
            device_id={"tp": peer},
            device_id_type=MESH,
        ).wait_recv()
    whole = jnp.sum(squares[...], axis=0)[0:1]
    inverse = lax.rsqrt(whole / WIDTH + epsilon)
    inverse = jnp.broadcast_to(inverse, (128, TOK)).T
    inverse = jnp.concatenate([inverse] * (PIECE // 128), axis=1)
    for copy in weights:
        copy.wait()

    def use(source, owner, start):
        gain = gain_ref[pl.ds(owner, 1), :]
        normed = (source[...].astype(jnp.float32) * inverse * gain).astype(jnp.bfloat16)
        rows = pl.ds(pl.multiple_of(owner * PIECE, PIECE), PIECE)
        product = jnp.dot(normed, w[rows, :], preferred_element_type=jnp.float32)
        if start:
            acc[...] = product
        else:
            acc[...] += product

    use(h_ref, t, True)
    for i in range(CH):
        arrived(down, upward[i])
        if i < 2:
            send(gath.at[down, part(upward[i])], down, upward[i], up)
        arrived(up, downward[i])
        if i < 2:
            send(gath.at[up, part(downward[i])], up, downward[i], down)
        arrived(across, upward[i])
        if i == 1:
            for chunk in (0, 1):
                send(gath.at[across, part(chunk)], across, chunk, up)
                send(gath.at[across, part(chunk)], across, chunk, down)
        if i > 1:
            send(gath.at[across, part(i)], across, i, up)
            send(gath.at[across, part(i)], across, i, down)
    use(gath.at[up], up, False)
    use(gath.at[down], down, False)
    for i in range(2):
        for chunk in (upward[i], downward[i]):
            arrived(far, chunk)
            send(gath.at[far, part(chunk)], far, chunk, across)
    use(gath.at[across], across, False)
    use(gath.at[far], far, False)
    for chunk in (0, 2, 1, 3):
        arrived(other(far), chunk)
    use(gath.at[other(far)], other(far), False)
    for side in (up, down):
        for chunk in range(CH):
            arrived(other(side), chunk)
        use(gath.at[other(side)], other(side), False)

    half = HEAD_SIZE // 2
    for head in range(GROUP + 1):
        raw = acc[:, head * HEAD_SIZE : (head + 1) * HEAD_SIZE].T
        a = raw[:half]
        b = raw[half:]
        low = a * cosine[...] - b * sine[...]
        high = b * cosine[...] + a * sine[...]
        if head < GROUP:
            cols = slice(head * TOK, (head + 1) * TOK)
            q_out[0:half, cols] = (low * SCALE).astype(jnp.bfloat16)
            q_out[half:, cols] = (high * SCALE).astype(jnp.bfloat16)
        else:
            turned = jnp.concatenate([low, high], axis=0).T
            kv_out[0:TOK, :] = turned.astype(jnp.bfloat16)
    value = acc[:, (GROUP + 1) * HEAD_SIZE :].T.astype(jnp.bfloat16)
    for i in range(TOK // 128):
        kv_out[TOK + 128 * i : TOK + 128 * (i + 1), :] = value[:, 128 * i : 128 * (i + 1)]
    lane = lax.broadcasted_iota(jnp.int32, (16, 128), 1)
    row = lax.broadcasted_iota(jnp.int32, (16, 128), 0)
    tail = jnp.zeros((16, 128), jnp.int32)
    for d in range(1, DOCS):
        count = jnp.sum(jnp.where(doc_ref[...] < d, 1, 0), axis=1, keepdims=True)
        tail = jnp.where(
            (lane == d) & (row == 0), count // 16, jnp.where((lane == d) & (row == 1), count % 16, tail)
        )
    kv_out[2 * TOK :, :] = tail.astype(jnp.float32).astype(jnp.bfloat16)
    for copy in sent + told:
        copy.wait_send()


def project(hidden, norm_gain, w_query, w_key, w_value, doc_ids):
    vmem = pl.BlockSpec(memory_space=pltpu.VMEM)
    hbm = pl.BlockSpec(memory_space=pl.ANY)
    powers = -np.arange(HEAD_SIZE // 2, dtype=np.float32) * np.float32(2.0) / HEAD_SIZE
    freqs = (np.float64(rope_base) ** powers.astype(np.float64)).astype(np.float32)
    freqs = jnp.asarray(np.broadcast_to(freqs[:, None], (HEAD_SIZE // 2, TOK)))
    return pl.pallas_call(
        project_kernel,
        out_shape=(
            jax.ShapeDtypeStruct((HEAD_SIZE, ROWS), jnp.bfloat16),
            jax.ShapeDtypeStruct((BLK, 128), jnp.bfloat16),
        ),
        in_specs=[vmem] * 4 + [hbm] * 3,
        out_specs=(vmem, vmem),
        scratch_shapes=[
            pltpu.VMEM((N_TP, TOK, PIECE), jnp.bfloat16),
            pltpu.VMEM((WIDTH, 768), jnp.bfloat16),
            pltpu.VMEM((TOK, 768), jnp.float32),
            pltpu.VMEM((N_TP, 8, TOK), jnp.float32),
            pltpu.VMEM((HEAD_SIZE // 2, TOK), jnp.float32),
            pltpu.VMEM((HEAD_SIZE // 2, TOK), jnp.float32),
            pltpu.SemaphoreType.DMA((3,)),
            pltpu.SemaphoreType.DMA((28,)),
            pltpu.SemaphoreType.DMA((N_TP, CH)),
            pltpu.SemaphoreType.DMA((N_TP - 1,)),
            pltpu.SemaphoreType.DMA((N_TP,)),
        ],
        compiler_params=pltpu.CompilerParams(
            collective_id=0, has_side_effects=True, vmem_limit_bytes=48 * 2**20
        ),
        name="project",
    )(hidden, norm_gain.reshape(N_TP, PIECE), freqs, doc_ids, w_query, w_key, w_value)


def combine_kernel(
    att, w_out, out_ref,
    w, terms, sums, across_in, side_in, half_in, side_end, across_end,
    wsem, ssem, rsem,
):
    t, up, down, far = tp_places()
    across = other(t)
    order = [other(far), other(up), other(down), far, across, up, down, t]
    weights = []
    for i, owner in enumerate(order):
        cols = pl.ds(pl.multiple_of(owner * PIECE, PIECE), PIECE)
        weights.append(pltpu.make_async_copy(w_out.at[:, cols], w.at[i], wsem.at[i]))
        weights[-1].start()
    greet("tp", (up, down, across))
    sent = []

    def send(source, target, number, to):
        copy = pltpu.make_async_remote_copy(
            src_ref=source,
            dst_ref=target,
            send_sem=ssem.at[len(sent)],
            recv_sem=rsem.at[number],
            device_id={"tp": to},
            device_id_type=MESH,
        )
        copy.start()
        sent.append(copy)

    def arrived(target, number):
        pltpu.make_async_remote_copy(
            src_ref=target,
            dst_ref=target,
            send_sem=ssem.at[0],
            recv_sem=rsem.at[number],
            device_id={"tp": across},
            device_id_type=MESH,
        ).wait_recv()
        return target[...].astype(jnp.float32)

    def compute(i):
        weights[i].wait()
        product = jnp.dot(att[...], w[i], preferred_element_type=jnp.float32)
        terms[i] = product.astype(jnp.bfloat16)

    def term(i, chunk):
        return terms[i, part(chunk)].astype(jnp.float32)

    UP, DOWN = 0, 1
    compute(0)
    for chunk in (0, 2, 1, 3):
        send(terms.at[0, part(chunk)], across_in.at[part(chunk)], chunk, across)
    compute(1)
    compute(2)
    for chunk in range(CH):
        send(terms.at[1, part(chunk)], side_in.at[DOWN, part(chunk)], 4 + chunk, up)
        send(terms.at[2, part(chunk)], side_in.at[UP, part(chunk)], 8 + chunk, down)
    for i in range(3, 8):
        compute(i)
    for chunk in (0, 2, 1, 3):
        got = arrived(across_in.at[part(chunk)], chunk)
        sums[0, part(chunk)] = (term(3, chunk) + got).astype(jnp.bfloat16)
        if chunk < 2:
            send(sums.at[0, part(chunk)], half_in.at[DOWN, part(chunk)], 12 + chunk, up)
        else:
            send(sums.at[0, part(chunk)], half_in.at[UP, part(chunk - 2)], 12 + chunk, down)
    for chunk in range(CH):
        below = arrived(side_in.at[DOWN, part(chunk)], 4 + chunk)
        above = arrived(side_in.at[UP, part(chunk)], 8 + chunk)
        sums[1, part(chunk)] = (term(4, chunk) + below + above).astype(jnp.bfloat16)
        send(sums.at[1, part(chunk)], across_end.at[part(chunk)], 16 + chunk, across)
    for i in range(2):
        send(terms.at[5, part(2 + i)], side_end.at[DOWN, part(2 + i)], 22 + i, up)
        send(terms.at[6, part(i)], side_end.at[UP, part(i)], 24 + i, down)
    for i in range(2):
        got = arrived(half_in.at[DOWN, part(i)], 12 + i)
        sums[2, part(i)] = (term(5, i) + got).astype(jnp.bfloat16)
        send(sums.at[2, part(i)], side_end.at[DOWN, part(i)], 20 + i, up)
        got = arrived(half_in.at[UP, part(i)], 14 + i)
        sums[3, part(2 + i)] = (term(6, 2 + i) + got).astype(jnp.bfloat16)
        send(sums.at[3, part(2 + i)], side_end.at[UP, part(2 + i)], 26 + i, down)
    for chunk in range(CH):
        total = term(7, chunk) + arrived(across_end.at[part(chunk)], 16 + chunk)
        total = total + arrived(side_end.at[DOWN, part(chunk)], 20 + chunk)
        total = total + arrived(side_end.at[UP, part(chunk)], 24 + chunk)
        out_ref[part(chunk), :] = total.astype(jnp.bfloat16)
    for copy in sent:
        copy.wait_send()


def combine(attended, w_out):
    vmem = pl.BlockSpec(memory_space=pltpu.VMEM)
    hbm = pl.BlockSpec(memory_space=pl.ANY)
    return pl.pallas_call(
        combine_kernel,
        out_shape=jax.ShapeDtypeStruct((TOK, PIECE), jnp.bfloat16),
        in_specs=[vmem, hbm],
        out_specs=vmem,
        scratch_shapes=[
            pltpu.VMEM((N_TP, PIECE, PIECE), jnp.bfloat16),
            pltpu.VMEM((N_TP, TOK, PIECE), jnp.bfloat16),
            pltpu.VMEM((4, TOK, PIECE), jnp.bfloat16),
            pltpu.VMEM((TOK, PIECE), jnp.bfloat16),
            pltpu.VMEM((2, TOK, PIECE), jnp.bfloat16),
            pltpu.VMEM((2, TOK // 2, PIECE), jnp.bfloat16),
            pltpu.VMEM((2, TOK, PIECE), jnp.bfloat16),
            pltpu.VMEM((TOK, PIECE), jnp.bfloat16),
            pltpu.SemaphoreType.DMA((N_TP,)),
            pltpu.SemaphoreType.DMA((28,)),
            pltpu.SemaphoreType.DMA((28,)),
        ],
        compiler_params=pltpu.CompilerParams(
            collective_id=1, has_side_effects=True, vmem_limit_bytes=40 * 2**20
        ),
        name="combine",
    )(attended, w_out)


def augment_queries(q_ref, doc_ref, qaug):
    qaug[0:HEAD_SIZE, :] = q_ref[...]
    row = lax.broadcasted_iota(jnp.int32, (HEAD_SIZE, TOK), 0)
    hot = jnp.where(row == doc_ref[...], PENALTY, 0.0).astype(jnp.bfloat16)
    for head in range(GROUP):
        qaug[HEAD_SIZE:, head * TOK : (head + 1) * TOK] = hot


def attend_keys(block):
    counts = block[2 * TOK : 2 * TOK + 2, :].astype(jnp.float32)
    below = counts[0:1] * 16.0 + counts[1:2]
    row = lax.broadcasted_iota(jnp.int32, (TOK, HEAD_SIZE), 0).astype(jnp.float32)
    earlier = jnp.where(row < below, 1.0, 0.0).astype(jnp.bfloat16)
    return jnp.concatenate([block[0:TOK, :], earlier], axis=1)


def score(keys, chunk, slot, qaug, logits, tops, causal):
    cols = slice(chunk * QC, (chunk + 1) * QC)
    length = keys.shape[0]
    scores = jnp.dot(keys, qaug[:, cols], preferred_element_type=jnp.float32)
    if causal:
        key_at = lax.broadcasted_iota(jnp.int32, (TOK, QC), 0)
        query_at = lax.broadcasted_iota(jnp.int32, (TOK, QC), 1) + (chunk * QC) % TOK
        scores = jnp.where(key_at <= query_at, scores, jnp.float32(PENALTY))
    logits[slot, 0:length] = scores
    tops[slot] = jnp.max(scores, axis=0, keepdims=True)


def weigh(values, chunk, slot, logits, tops, best, acc, first):
    cols = slice(chunk * QC, (chunk + 1) * QC)
    top = tops[slot]
    if not first:
        old = best[:, cols]
        top = jnp.maximum(old, top)
    weights = jnp.exp2(logits[slot, 0 : values.shape[1]] - top).astype(jnp.bfloat16)
    out = jnp.dot(values, weights, preferred_element_type=jnp.float32)
    if first:
        acc[:, cols] = out
    else:
        acc[:, cols] = acc[:, cols] * jnp.exp2(old - top) + out
    best[:, cols] = top


def attend(blocks, state, first):
    qaug, logits, tops, best, acc = state
    chunks = ROWS // QC
    keys = jnp.concatenate([attend_keys(block) for block in blocks], axis=0)
    values = jnp.concatenate(
        [
            block[TOK + 128 * i : TOK + 128 * (i + 1), :]
            for block in blocks
            for i in range(TOK // 128)
        ],
        axis=1,
    )
    ones = jnp.ones((16, values.shape[1]), jnp.bfloat16)
    values = jnp.concatenate([values, ones], axis=0)
    score(keys, 0, 0, qaug, logits, tops, first)
    for chunk in range(chunks):
        if chunk + 1 < chunks:
            score(keys, chunk + 1, (chunk + 1) % 2, qaug, logits, tops, first)
        weigh(values, chunk, chunk % 2, logits, tops, best, acc, first)


def finish(acc, out_ref):
    for head in range(GROUP):
        cols = slice(head * TOK, (head + 1) * TOK)
        total = acc[HEAD_SIZE : HEAD_SIZE + 1, cols]
        out_ref[:, head * HEAD_SIZE : (head + 1) * HEAD_SIZE] = (
            (acc[0:HEAD_SIZE, cols] / total).T.astype(jnp.bfloat16)
        )


ROLES = 15
PARTS = ((0, TOK), (TOK, TOK + 16))
PROGRAM = [
    (0, [(0, 0), (0, 1), (15, 0), (15, 1)]),
    (2, [(2, 0), (2, 1), (3, 0), (4, 0)]),
    (1, [(1, 0), (1, 1), (3, 1), (4, 1)]),
    (3, []),
    (4, [(5, 0), (6, 0)]),
    (5, [(5, 1), (6, 1)]),
    (6, [(11, 0), (7, 0)]),
    (9, [(9, 0), (9, 1)]),
    (8, [(8, 0), (8, 1)]),
    (11, [(12, 0), (13, 0), (11, 1), (7, 1)]),
    (7, []),
    (12, [(12, 1), (13, 1)]),
    (13, [(10, 0), (10, 1)]),
    (10, [(14, 0), (14, 1)]),
    (14, []),
]


def attention_kernel(
    q_ref, doc_ref, own_ref, out_ref,
    kv, qaug, logits, tops, best, acc, ssem, rsem, sibsend, sibrecv,
):
    me = lax.axis_index("cp")
    core = me % 2
    x = (me // 2) % 4
    z = me // 8
    state = (qaug, logits, tops, best, acc)

    def at(zz, xx):
        return (zz * 4 + xx) * 2 + core

    right = at(z, (x + 1) % 4)
    left = at(z, (x + 3) % 4)
    ahead = at((z + 1) % 4, x)
    behind = at((z + 3) % 4, x)
    sibling = me + 1 - 2 * core
    greet("cp", (right, left, ahead, behind, sibling))

    def move(source, slot, half, to, send_sem, recv_sem):
        rows = pl.ds(*PARTS[half])
        return pltpu.make_async_remote_copy(
            src_ref=source.at[rows],
            dst_ref=kv.at[slot, rows],
            send_sem=send_sem,
            recv_sem=recv_sem,
            device_id={"cp": to},
            device_id_type=MESH,
        )

    always = z >= 0
    top = z == 3
    one, two = z >= 1, z >= 2
    xm, xp, x2 = (x + 3) % 4, (x + 1) % 4, (x + 2) % 4
    roles = [
        (x >= 1, z, xm),
        (x == 3, z, xp),
        (x >= 2, z, x2),
        (one, (z + 3) % 4, x),
        (top, 0 * z, x),
        (one, (z + 3) % 4, xm),
        (one, (z + 3) % 4, xp),
        (top & (x < 3), 0 * z, xp),
        (top & (x == 0), 0 * z, xm),
        (one, (z + 3) % 4, x2),
        (top & (x < 2), 0 * z, x2),
        (two, (z + 2) % 4, x),
        (two, (z + 2) % 4, xm),
        (two, (z + 2) % 4, xp),
        (two, (z + 2) % 4, x2),
        ((z == 0) & (x < 3), z, xp),
    ]
    slots = [at(zz, xx) for _, zz, xx in roles]
    middle = (x == 1) | (x == 2)
    forwards = {
        0: [(middle, right, (0, 1))],
        3: [(z < 3, ahead, (0, 1)), (always, right, (0, 1)), (always, left, (1, 0))],
        4: [(x == 3, right, (0, 1))],
        5: [(always, right, (0,))],
        6: [(always, left, (1,))],
        7: [(middle, left, (0, 1))],
        15: [(always, behind, (0, 1))],
        11: [(always, right, (0, 1)), (always, left, (1, 0))],
        12: [(always, right, (0,))],
        13: [(always, left, (1,))],
    }
    sends = []

    def plan(when, source, slot, half, to):
        number = len(sends)
        sends.append((when, source, slot, half, to))
        return number

    def issue(number):
        when, source, slot, half, to = sends[number]

        @pl.when(when)
        def _():
            move(source, slot, half, to, ssem.at[number], rsem.at[slot, half]).start()

    own = []
    for half in (0, 1):
        own.append(plan(z < 3, own_ref, me, half, ahead))
        own.append(plan(z == 0, own_ref, me, half, behind))
        own.append(plan(x < 3, own_ref, me, half, right))
        own.append(plan((x == 0) | (z == 0), own_ref, me, half, left))
    relays = {}
    for role, targets in forwards.items():
        relays[role] = {0: [], 1: []}
        for when, to, halves in targets:
            for half in halves:
                number = plan(roles[role][0] & when, kv.at[slots[role]], slots[role], half, to)
                relays[role][half].append(number)

    for half in (0, 1):
        move(own_ref, me, half, sibling, sibsend.at[ROLES, half], sibrecv.at[ROLES, half]).start()
    for number in own:
        issue(number)
    augment_queries(q_ref, doc_ref, qaug)
    attend([own_ref], state, True)
    for half in (0, 1):
        move(own_ref, sibling, half, sibling, sibsend.at[ROLES, half], sibrecv.at[ROLES, half]).wait_recv()

    @pl.when(core == 1)
    def _():
        attend([kv.at[sibling]], state, False)

    def serve(role, half):
        slot = slots[role]

        @pl.when(roles[role][0])
        def _():
            move(own_ref, slot, half, sibling, ssem.at[0], rsem.at[slot, half]).wait_recv()
            if role < ROLES:
                move(
                    kv.at[slot], slot, half, sibling, sibsend.at[role, half], sibrecv.at[role, half]
                ).start()

        for number in relays.get(role, {0: [], 1: []})[half]:
            issue(number)

    @pl.loop(0, ROLES)
    def _(step):
        there = step < 0
        slot = 0 * step
        turn = 0 * step
        for index, (role, services) in enumerate(PROGRAM):

            @pl.when(step == index)
            def _():
                for service in services:
                    serve(*service)

            there = there | ((step == index) & roles[role][0])
            slot = jnp.where(step == index, slots[role], slot)
            turn = jnp.where(step == index, role, turn)

        @pl.when(there)
        def _():
            twin = slot + 1 - 2 * core
            for half in (0, 1):
                move(own_ref, twin, half, sibling, sibsend.at[turn, half], sibrecv.at[turn, half]).wait_recv()
            attend([kv.at[slot], kv.at[twin]], state, False)

    finish(acc, out_ref)
    for number, (when, source, slot, half, to) in enumerate(sends):

        @pl.when(when)
        def _():
            move(source, slot, half, to, ssem.at[number], rsem.at[slot, half]).wait_send()

    for role in range(ROLES + 1):
        present, slot = (always, me) if role == ROLES else (roles[role][0], slots[role])
        for half in (0, 1):

            @pl.when(present)
            def _():
                move(
                    own_ref, slot, half, sibling, sibsend.at[role, half], sibrecv.at[role, half]
                ).wait_send()


SENDS = 30


def attention(queries, docs, block):
    vmem = pl.BlockSpec(memory_space=pltpu.VMEM)
    return pl.pallas_call(
        attention_kernel,
        out_shape=jax.ShapeDtypeStruct((TOK, GROUP * HEAD_SIZE), jnp.bfloat16),
        in_specs=[vmem] * 3,
        out_specs=vmem,
        scratch_shapes=[
            pltpu.VMEM((32, BLK, 128), jnp.bfloat16),
            pltpu.VMEM((2 * HEAD_SIZE, ROWS), jnp.bfloat16),
            pltpu.VMEM((2, 2 * TOK, QC), jnp.float32),
            pltpu.VMEM((2, 1, QC), jnp.float32),
            pltpu.VMEM((1, ROWS), jnp.float32),
            pltpu.VMEM((HEAD_SIZE + 16, ROWS), jnp.float32),
            pltpu.SemaphoreType.DMA((SENDS,)),
            pltpu.SemaphoreType.DMA((32, 2)),
            pltpu.SemaphoreType.DMA((ROLES + 1, 2)),
            pltpu.SemaphoreType.DMA((ROLES + 1, 2)),
        ],
        compiler_params=pltpu.CompilerParams(
            collective_id=2, has_side_effects=True, vmem_limit_bytes=40 * 2**20
        ),
        name="attention",
    )(queries, docs, block)


def shards(hidden, norm_gain, w_query, w_key, w_value, w_out, doc_ids):
    docs = doc_ids.reshape(1, TOK)
    queries, block = project(hidden, norm_gain, w_query, w_key, w_value, docs)
    attended = attention(queries, docs, block)
    return combine(attended, w_out)


def solution(mesh):
    in_specs = (
        P("cp", "tp"),
        P(),
        P(None, "tp"),
        P(None, "tp"),
        P(None, "tp"),
        P("tp", None),
        P("cp"),
    )
    return jax.shard_map(
        shards, mesh=mesh, in_specs=in_specs, out_specs=P("cp", "tp"), check_vma=False
    )
```

```python
import math

import jax
import jax.numpy as jnp
import numpy as np
from jax import lax
from jax.experimental import pallas as pl
from jax.experimental.pallas import tpu as pltpu
from jax.sharding import PartitionSpec as P

HEADS = 32
KV_HEADS = 8
HEAD_SIZE = 128
LONGEST = 12288
DOCS = 6
TOK = 512
GROUP = 4
ROWS = GROUP * TOK
BLK = 2 * TOK + 16
PENALTY = -(2.0**100)
SCALE = math.log2(math.e) / math.sqrt(HEAD_SIZE)
QC = 512

epsilon = 1e-05
rope_base = 500000.0


WIDTH = 4096
PIECE = 512
N_TP = 8
CH = 4
CR = TOK // CH
MESH = pl.DeviceIdType.MESH


def tp_places():
    t = lax.axis_index("tp")
    plane = (t // 4) * 4
    y = t % 4
    up = plane + (y + 1) % 4
    down = plane + (y + 3) % 4
    far = plane + (y + 2) % 4
    return t, up, down, far


def other(t):
    return (t + 4) % 8


def part(chunk):
    return pl.ds(chunk * CR, CR)


def projection(
    h_ref, gain_ref, freq_ref, doc_ref, weights, inputs, q_out, kv_out, begin,
    gath, w, acc, squares, cosine, sine, ssem, rsem, qssem, qrsem,
):
    t, up, down, far = tp_places()
    across = other(t)
    peers = [(t + i) % N_TP for i in range(1, N_TP)]
    for copy in inputs:
        copy.wait()
    sent = []

    def send(source, owner, chunk, to):
        copy = pltpu.make_async_remote_copy(
            src_ref=source,
            dst_ref=gath.at[owner, part(chunk)],
            send_sem=ssem.at[len(sent)],
            recv_sem=rsem.at[owner, chunk],
            device_id={"tp": to},
            device_id_type=MESH,
        )
        copy.start()
        sent.append(copy)

    def arrived(owner, chunk):
        pltpu.make_async_remote_copy(
            src_ref=gath.at[owner, part(chunk)],
            dst_ref=gath.at[owner, part(chunk)],
            send_sem=ssem.at[0],
            recv_sem=rsem.at[owner, chunk],
            device_id={"tp": across},
            device_id_type=MESH,
        ).wait_recv()

    upward = (0, 1, 2, 3)
    downward = (2, 3, 0, 1)

    def send_own(i):
        send(h_ref.at[part(upward[i])], t, upward[i], up)
        send(h_ref.at[part(downward[i])], t, downward[i], down)
        send(h_ref.at[part(upward[i])], t, upward[i], across)

    send_own(0)
    mine = h_ref[...].astype(jnp.float32)
    mass = jnp.sum(mine * mine, axis=1, keepdims=True)
    squares[t] = jnp.broadcast_to(mass, (TOK, 128)).T[0:8]
    told = []
    for i, peer in enumerate(peers):
        copy = pltpu.make_async_remote_copy(
            src_ref=squares.at[t],
            dst_ref=squares.at[t],
            send_sem=qssem.at[i],
            recv_sem=qrsem.at[t],
            device_id={"tp": peer},
            device_id_type=MESH,
        )
        copy.start()
        told.append(copy)
    for i in range(1, CH):
        send_own(i)

    first = lax.axis_index("cp") * TOK
    place = (first + lax.broadcasted_iota(jnp.int32, (HEAD_SIZE // 2, TOK), 1)).astype(jnp.float32)
    angle = place * jnp.concatenate([freq_ref[...]] * (TOK // 128), axis=1)
    cosine[...] = jnp.cos(angle)
    sine[...] = jnp.sin(angle)
    for peer in peers:
        pltpu.make_async_remote_copy(
            src_ref=squares.at[peer],
            dst_ref=squares.at[peer],
            send_sem=qssem.at[0],
            recv_sem=qrsem.at[peer],
            device_id={"tp": peer},
            device_id_type=MESH,
        ).wait_recv()
    whole = jnp.sum(squares[...], axis=0)[0:1]
    inverse = lax.rsqrt(whole / WIDTH + epsilon)
    inverse = jnp.broadcast_to(inverse, (128, TOK)).T
    inverse = jnp.concatenate([inverse] * (PIECE // 128), axis=1)
    for copy in weights:
        copy.wait()

    def use(source, owner, start):
        gain = gain_ref[:, pl.ds(pl.multiple_of(owner * PIECE, PIECE), PIECE)]
        normed = (source[...].astype(jnp.float32) * inverse * gain).astype(jnp.bfloat16)
        rows = pl.ds(pl.multiple_of(owner * PIECE, PIECE), PIECE)
        product = jnp.dot(normed, w[rows, :], preferred_element_type=jnp.float32)
        if start:
            acc[...] = product
        else:
            acc[...] += product

    use(h_ref, t, True)
    for i in range(CH):
        arrived(down, upward[i])
        if i < 2:
            send(gath.at[down, part(upward[i])], down, upward[i], up)
        arrived(up, downward[i])
        if i < 2:
            send(gath.at[up, part(downward[i])], up, downward[i], down)
        arrived(across, upward[i])
        if i == 1:
            for chunk in (0, 1):
                send(gath.at[across, part(chunk)], across, chunk, up)
                send(gath.at[across, part(chunk)], across, chunk, down)
        if i > 1:
            send(gath.at[across, part(i)], across, i, up)
            send(gath.at[across, part(i)], across, i, down)
    use(gath.at[up], up, False)
    use(gath.at[down], down, False)
    for i in range(2):
        for chunk in (upward[i], downward[i]):
            arrived(far, chunk)
            send(gath.at[far, part(chunk)], far, chunk, across)
    use(gath.at[across], across, False)
    use(gath.at[far], far, False)
    for chunk in (0, 2, 1, 3):
        arrived(other(far), chunk)
    use(gath.at[other(far)], other(far), False)
    for side in (up, down):
        for chunk in range(CH):
            arrived(other(side), chunk)
        use(gath.at[other(side)], other(side), False)

    half = HEAD_SIZE // 2

    def rotated(head):
        raw = acc[:, head * HEAD_SIZE : (head + 1) * HEAD_SIZE].T
        low = raw[:half] * cosine[...] - raw[half:] * sine[...]
        high = raw[half:] * cosine[...] + raw[:half] * sine[...]
        return low, high

    low, high = rotated(GROUP)
    kv_out[0:TOK, :] = jnp.concatenate([low, high], axis=0).T.astype(jnp.bfloat16)
    value = acc[:, (GROUP + 1) * HEAD_SIZE :].T.astype(jnp.bfloat16)
    for i in range(TOK // 128):
        kv_out[TOK + 128 * i : TOK + 128 * (i + 1), :] = value[:, 128 * i : 128 * (i + 1)]
    lane = lax.broadcasted_iota(jnp.int32, (16, 128), 1)
    row = lax.broadcasted_iota(jnp.int32, (16, 128), 0)
    tail = jnp.zeros((16, 128), jnp.int32)
    for d in range(1, DOCS):
        count = jnp.sum(jnp.where(doc_ref[...] < d, 1, 0), axis=1, keepdims=True)
        tail = jnp.where(
            (lane == d) & (row == 0), count // 16, jnp.where((lane == d) & (row == 1), count % 16, tail)
        )
    kv_out[2 * TOK :, :] = tail.astype(jnp.float32).astype(jnp.bfloat16)
    begin()
    for head in range(GROUP):
        low, high = rotated(head)
        cols = slice(head * TOK, (head + 1) * TOK)
        q_out[0:half, cols] = (low * SCALE).astype(jnp.bfloat16)
        q_out[half:HEAD_SIZE, cols] = (high * SCALE).astype(jnp.bfloat16)
    return sent + told


def combination(
    att, out_ref, weights, w, terms, sums, across_in, side_in, half_in, side_end, across_end, ssem, rsem,
):
    t, up, down, far = tp_places()
    across = other(t)
    sent = []

    def send(source, target, number, to):
        copy = pltpu.make_async_remote_copy(
            src_ref=source,
            dst_ref=target,
            send_sem=ssem.at[len(sent)],
            recv_sem=rsem.at[number],
            device_id={"tp": to},
            device_id_type=MESH,
        )
        copy.start()
        sent.append(copy)

    def arrived(target, number):
        pltpu.make_async_remote_copy(
            src_ref=target,
            dst_ref=target,
            send_sem=ssem.at[0],
            recv_sem=rsem.at[number],
            device_id={"tp": across},
            device_id_type=MESH,
        ).wait_recv()
        return target[...].astype(jnp.float32)

    def compute(i):
        weights[i].wait()
        product = jnp.dot(att[...], w[i], preferred_element_type=jnp.float32)
        terms[i] = product.astype(jnp.bfloat16)

    def term(i, chunk):
        return terms[i, part(chunk)].astype(jnp.float32)

    UP, DOWN = 0, 1
    compute(0)
    for chunk in (0, 2, 1, 3):
        send(terms.at[0, part(chunk)], across_in.at[part(chunk)], chunk, across)
    compute(1)
    compute(2)
    for chunk in range(CH):
        send(terms.at[1, part(chunk)], side_in.at[DOWN, part(chunk)], 4 + chunk, up)
        send(terms.at[2, part(chunk)], side_in.at[UP, part(chunk)], 8 + chunk, down)
    for i in range(3, 8):
        compute(i)
    for chunk in (0, 2, 1, 3):
        got = arrived(across_in.at[part(chunk)], chunk)
        sums[0, part(chunk)] = (term(3, chunk) + got).astype(jnp.bfloat16)
        if chunk < 2:
            send(sums.at[0, part(chunk)], half_in.at[DOWN, part(chunk)], 12 + chunk, up)
        else:
            send(sums.at[0, part(chunk)], half_in.at[UP, part(chunk - 2)], 12 + chunk, down)
    for chunk in range(CH):
        below = arrived(side_in.at[DOWN, part(chunk)], 4 + chunk)
        above = arrived(side_in.at[UP, part(chunk)], 8 + chunk)
        sums[1, part(chunk)] = (term(4, chunk) + below + above).astype(jnp.bfloat16)
        send(sums.at[1, part(chunk)], across_end.at[part(chunk)], 16 + chunk, across)
    for i in range(2):
        send(terms.at[5, part(2 + i)], side_end.at[DOWN, part(2 + i)], 22 + i, up)
        send(terms.at[6, part(i)], side_end.at[UP, part(i)], 24 + i, down)
    for i in range(2):
        got = arrived(half_in.at[DOWN, part(i)], 12 + i)
        sums[2, part(i)] = (term(5, i) + got).astype(jnp.bfloat16)
        send(sums.at[2, part(i)], side_end.at[DOWN, part(i)], 20 + i, up)
        got = arrived(half_in.at[UP, part(i)], 14 + i)
        sums[3, part(2 + i)] = (term(6, 2 + i) + got).astype(jnp.bfloat16)
        send(sums.at[3, part(2 + i)], side_end.at[UP, part(2 + i)], 26 + i, down)
    for chunk in range(CH):
        total = term(7, chunk) + arrived(across_end.at[part(chunk)], 16 + chunk)
        total = total + arrived(side_end.at[DOWN, part(chunk)], 20 + chunk)
        total = total + arrived(side_end.at[UP, part(chunk)], 24 + chunk)
        out_ref[part(chunk), :] = total.astype(jnp.bfloat16)
    return sent


def augment_queries(doc_ref, qaug):
    row = lax.broadcasted_iota(jnp.int32, (HEAD_SIZE, TOK), 0)
    hot = jnp.where(row == doc_ref[...], PENALTY, 0.0).astype(jnp.bfloat16)
    for head in range(GROUP):
        qaug[HEAD_SIZE:, head * TOK : (head + 1) * TOK] = hot


def attend_keys(block):
    counts = block[2 * TOK : 2 * TOK + 2, :].astype(jnp.float32)
    below = counts[0:1] * 16.0 + counts[1:2]
    row = lax.broadcasted_iota(jnp.int32, (TOK, HEAD_SIZE), 0).astype(jnp.float32)
    earlier = jnp.where(row < below, 1.0, 0.0).astype(jnp.bfloat16)
    return jnp.concatenate([block[0:TOK, :], earlier], axis=1)


def score(keys, chunk, slot, qaug, logits, tops, causal):
    cols = slice(chunk * QC, (chunk + 1) * QC)
    length = keys.shape[0]
    scores = jnp.dot(keys, qaug[:, cols], preferred_element_type=jnp.float32)
    if causal:
        key_at = lax.broadcasted_iota(jnp.int32, (TOK, QC), 0)
        query_at = lax.broadcasted_iota(jnp.int32, (TOK, QC), 1) + (chunk * QC) % TOK
        scores = jnp.where(key_at <= query_at, scores, jnp.float32(PENALTY))
    logits[slot, 0:length] = scores
    tops[slot] = jnp.max(scores, axis=0, keepdims=True)


def weigh(values, chunk, slot, logits, tops, best, acc, first):
    cols = slice(chunk * QC, (chunk + 1) * QC)
    top = tops[slot]
    if not first:
        old = best[:, cols]
        top = jnp.maximum(old, top)
    weights = jnp.exp2(logits[slot, 0 : values.shape[1]] - top).astype(jnp.bfloat16)
    out = jnp.dot(values, weights, preferred_element_type=jnp.float32)
    if first:
        acc[:, cols] = out
    else:
        acc[:, cols] = acc[:, cols] * jnp.exp2(old - top) + out
    best[:, cols] = top


def attend(blocks, state, first):
    qaug, logits, tops, best, acc = state
    chunks = ROWS // QC
    keys = jnp.concatenate([attend_keys(block) for block in blocks], axis=0)
    values = jnp.concatenate(
        [
            block[TOK + 128 * i : TOK + 128 * (i + 1), :]
            for block in blocks
            for i in range(TOK // 128)
        ],
        axis=1,
    )
    ones = jnp.ones((16, values.shape[1]), jnp.bfloat16)
    values = jnp.concatenate([values, ones], axis=0)
    score(keys, 0, 0, qaug, logits, tops, first)
    for chunk in range(chunks):
        if chunk + 1 < chunks:
            score(keys, chunk + 1, (chunk + 1) % 2, qaug, logits, tops, first)
        weigh(values, chunk, chunk % 2, logits, tops, best, acc, first)


def finish(acc, out_ref):
    for head in range(GROUP):
        cols = slice(head * TOK, (head + 1) * TOK)
        total = acc[HEAD_SIZE : HEAD_SIZE + 1, cols]
        out_ref[:, head * HEAD_SIZE : (head + 1) * HEAD_SIZE] = (
            (acc[0:HEAD_SIZE, cols] / total).T.astype(jnp.bfloat16)
        )


ROLES = 15
PARTS = ((0, TOK), (TOK, TOK + 16))
PROGRAM = [
    (0, [(0, 0), (0, 1), (15, 0), (15, 1)]),
    (2, [(2, 0), (2, 1), (3, 0), (4, 0)]),
    (1, [(1, 0), (1, 1), (3, 1), (4, 1)]),
    (3, []),
    (4, [(5, 0), (6, 0)]),
    (5, [(5, 1), (6, 1)]),
    (6, [(11, 0), (7, 0)]),
    (9, [(9, 0), (9, 1)]),
    (8, [(8, 0), (8, 1)]),
    (11, [(11, 1), (12, 0), (13, 0), (7, 1)]),
    (7, []),
    (12, [(12, 1), (13, 1)]),
    (13, [(10, 0), (10, 1)]),
    (10, [(14, 0), (14, 1)]),
    (14, []),
]


def attention(
    doc_ref, own_ref, out_ref, kv, qaug, logits, tops, best, acc, ssem, rsem, sibsend, sibrecv,
):
    me = lax.axis_index("cp")
    core = me % 2
    x = (me // 2) % 4
    z = me // 8
    state = (qaug, logits, tops, best, acc)

    def at(zz, xx):
        return (zz * 4 + xx) * 2 + core

    right = at(z, (x + 1) % 4)
    left = at(z, (x + 3) % 4)
    ahead = at((z + 1) % 4, x)
    behind = at((z + 3) % 4, x)
    sibling = me + 1 - 2 * core

    def move(source, slot, half, to, send_sem, recv_sem):
        rows = pl.ds(*PARTS[half])
        return pltpu.make_async_remote_copy(
            src_ref=source.at[rows],
            dst_ref=kv.at[slot, rows],
            send_sem=send_sem,
            recv_sem=recv_sem,
            device_id={"cp": to},
            device_id_type=MESH,
        )

    always = z >= 0
    top = z == 3
    one, two = z >= 1, z >= 2
    xm, xp, x2 = (x + 3) % 4, (x + 1) % 4, (x + 2) % 4
    roles = [
        (x >= 1, z, xm),
        (x == 3, z, xp),
        (x >= 2, z, x2),
        (one, (z + 3) % 4, x),
        (top, 0 * z, x),
        (one, (z + 3) % 4, xm),
        (one, (z + 3) % 4, xp),
        (top & (x < 3), 0 * z, xp),
        (top & (x == 0), 0 * z, xm),
        (one, (z + 3) % 4, x2),
        (top & (x < 2), 0 * z, x2),
        (two, (z + 2) % 4, x),
        (two, (z + 2) % 4, xm),
        (two, (z + 2) % 4, xp),
        (two, (z + 2) % 4, x2),
        ((z == 0) & (x < 3), z, xp),
    ]
    slots = [at(zz, xx) for _, zz, xx in roles]
    middle = (x == 1) | (x == 2)
    forwards = {
        0: [(middle, right, (0, 1))],
        3: [(z < 3, ahead, (0, 1)), (always, right, (0, 1)), (always, left, (1, 0))],
        4: [(x == 3, right, (0, 1))],
        5: [(always, right, (0,))],
        6: [(always, left, (1,))],
        7: [(middle, left, (0, 1))],
        15: [(always, behind, (0, 1))],
        11: [(always, right, (0, 1)), (always, left, (1, 0))],
        12: [(always, right, (0,))],
        13: [(always, left, (1,))],
    }
    sends = []

    def plan(when, source, slot, half, to):
        number = len(sends)
        sends.append((when, source, slot, half, to))
        return number

    def issue(number):
        when, source, slot, half, to = sends[number]

        @pl.when(when)
        def _():
            move(source, slot, half, to, ssem.at[number], rsem.at[slot, half]).start()

    own = []
    for half in (0, 1):
        own.append(plan(z < 3, own_ref, me, half, ahead))
        own.append(plan(z == 0, own_ref, me, half, behind))
        own.append(plan(x < 3, own_ref, me, half, right))
        own.append(plan((x == 0) | (z == 0), own_ref, me, half, left))
    relays = {}
    for role, targets in forwards.items():
        relays[role] = {0: [], 1: []}
        for when, to, halves in targets:
            for half in halves:
                number = plan(roles[role][0] & when, kv.at[slots[role]], slots[role], half, to)
                relays[role][half].append(number)

    def begin():
        for number in own:
            issue(number)
        for half in (0, 1):
            move(own_ref, me, half, sibling, sibsend.at[ROLES, half], sibrecv.at[ROLES, half]).start()

    def serve(role, half):
        slot = slots[role]

        @pl.when(roles[role][0])
        def _():
            move(own_ref, slot, half, sibling, ssem.at[0], rsem.at[slot, half]).wait_recv()
            if role < ROLES:
                move(
                    kv.at[slot], slot, half, sibling, sibsend.at[role, half], sibrecv.at[role, half]
                ).start()

        for number in relays.get(role, {0: [], 1: []})[half]:
            issue(number)

    def run():
        augment_queries(doc_ref, qaug)
        attend([own_ref], state, True)
        for half in (0, 1):
            move(own_ref, sibling, half, sibling, sibsend.at[ROLES, half], sibrecv.at[ROLES, half]).wait_recv()

        @pl.when(core == 1)
        def _():
            attend([kv.at[sibling]], state, False)

        @pl.loop(0, ROLES)
        def _(step):
            there = step < 0
            slot = 0 * step
            turn = 0 * step
            for index, (role, services) in enumerate(PROGRAM):

                @pl.when(step == index)
                def _():
                    for service in services:
                        serve(*service)

                there = there | ((step == index) & roles[role][0])
                slot = jnp.where(step == index, slots[role], slot)
                turn = jnp.where(step == index, role, turn)

            @pl.when(there)
            def _():
                twin = slot + 1 - 2 * core
                for half in (0, 1):
                    move(own_ref, twin, half, sibling, sibsend.at[turn, half], sibrecv.at[turn, half]).wait_recv()
                attend([kv.at[slot], kv.at[twin]], state, False)

        finish(acc, out_ref)

    def drain():
        for number, (when, source, slot, half, to) in enumerate(sends):

            @pl.when(when)
            def _():
                move(source, slot, half, to, ssem.at[number], rsem.at[slot, half]).wait_send()

        for role in range(ROLES + 1):
            present, slot = (always, me) if role == ROLES else (roles[role][0], slots[role])
            for half in (0, 1):

                @pl.when(present)
                def _():
                    move(
                        own_ref, slot, half, sibling, sibsend.at[role, half], sibrecv.at[role, half]
                    ).wait_send()

    return begin, run, drain


SENDS = 30
BF16, F32 = jnp.bfloat16, jnp.float32


def fused_kernel(
    h_hbm, gain_hbm, freq_hbm, doc_hbm, wq, wk, wv, w_out, out_ref,
    gath, w, pacc, squares, cosine, sine, gain_ref, freq_ref, doc_ref, insem, pssem, prsem, qssem, qrsem,
    own, kv, qaug, logits, tops, best, acc, assem, arsem, sibsend, sibrecv, att,
    wo, terms, sums, across_in, side_in, half_in, side_end, across_end, wosem, cssem, crsem,
):
    t, up, down, far = tp_places()
    across = other(t)
    me = lax.axis_index("cp")
    h_ref = gath.at[t]
    inputs = [
        pltpu.make_async_copy(h_hbm, h_ref, insem.at[0]),
        pltpu.make_async_copy(freq_hbm, freq_ref, insem.at[1]),
        pltpu.make_async_copy(gain_hbm, gain_ref, insem.at[2]),
        pltpu.make_async_copy(doc_hbm, doc_ref, insem.at[3]),
    ]
    weights = [
        pltpu.make_async_copy(wq, w.at[:, 0:512], insem.at[4]),
        pltpu.make_async_copy(wk, w.at[:, 512:640], insem.at[5]),
        pltpu.make_async_copy(wv, w.at[:, 640:768], insem.at[6]),
    ]
    order = [other(far), other(up), other(down), far, across, up, down, t]
    late = []
    for i, owner in enumerate(order):
        cols = pl.ds(pl.multiple_of(owner * PIECE, PIECE), PIECE)
        late.append(pltpu.make_async_copy(w_out.at[:, cols], wo.at[i], wosem.at[i]))
    for copy in inputs + weights + late:
        copy.start()
    core = me % 2
    column = (me // 2) % 4
    row = me // 8
    barrier = pltpu.get_barrier_semaphore()
    around = [
        me - me % 8 + (me + 2) % 8,
        me - me % 8 + (me + 6) % 8,
        (me + 8) % 32,
        (me + 24) % 32,
        me + 1 - 2 * core,
    ]
    for i in range(1, N_TP):
        pl.semaphore_signal(barrier, inc=1, device_id={"tp": (t + i) % N_TP}, device_id_type=MESH)
    for peer in around:
        pl.semaphore_signal(barrier, inc=1, device_id={"cp": peer}, device_id_type=MESH)
    pl.semaphore_wait(barrier, N_TP - 1 + len(around))

    begin, run, drain = attention(
        doc_ref, own, att, kv, qaug, logits, tops, best, acc, assem, arsem, sibsend, sibrecv
    )
    sent = projection(
        h_ref, gain_ref, freq_ref, doc_ref, weights, inputs, qaug, own, begin,
        gath, w, pacc, squares, cosine, sine, pssem, prsem, qssem, qrsem,
    )
    run()
    sent += combination(
        att, out_ref, late, wo, terms, sums, across_in, side_in, half_in, side_end, across_end, cssem, crsem
    )
    drain()
    for copy in sent:
        copy.wait_send()


def sublayer(hidden, norm_gain, w_query, w_key, w_value, w_out, doc_ids):
    hbm = pl.BlockSpec(memory_space=pl.ANY)
    powers = -np.arange(HEAD_SIZE // 2, dtype=np.float32) * np.float32(2.0) / HEAD_SIZE
    freqs = (np.float64(rope_base) ** powers.astype(np.float64)).astype(np.float32)
    freqs = jnp.asarray(np.broadcast_to(freqs[:, None], (HEAD_SIZE // 2, 128)))
    dma = pltpu.SemaphoreType.DMA
    return pl.pallas_call(
        fused_kernel,
        out_shape=jax.ShapeDtypeStruct((TOK, PIECE), BF16),
        in_specs=[hbm] * 8,
        out_specs=pl.BlockSpec(memory_space=pltpu.VMEM),
        scratch_shapes=[
            pltpu.VMEM((N_TP, TOK, PIECE), BF16),
            pltpu.VMEM((WIDTH, 768), BF16),
            pltpu.VMEM((TOK, 768), F32),
            pltpu.VMEM((N_TP, 8, TOK), F32),
            pltpu.VMEM((HEAD_SIZE // 2, TOK), F32),
            pltpu.VMEM((HEAD_SIZE // 2, TOK), F32),
            pltpu.VMEM((1, WIDTH), F32),
            pltpu.VMEM((HEAD_SIZE // 2, 128), F32),
            pltpu.VMEM((1, TOK), jnp.int32),
            dma((7,)),
            dma((28,)),
            dma((N_TP, CH)),
            dma((N_TP - 1,)),
            dma((N_TP,)),
            pltpu.VMEM((BLK, 128), BF16),
            pltpu.VMEM((32, BLK, 128), BF16),
            pltpu.VMEM((2 * HEAD_SIZE, ROWS), BF16),
            pltpu.VMEM((2, 2 * TOK, QC), F32),
            pltpu.VMEM((2, 1, QC), F32),
            pltpu.VMEM((1, ROWS), F32),
            pltpu.VMEM((HEAD_SIZE + 16, ROWS), F32),
            dma((SENDS,)),
            dma((32, 2)),
            dma((ROLES + 1, 2)),
            dma((ROLES + 1, 2)),
            pltpu.VMEM((TOK, GROUP * HEAD_SIZE), BF16),
            pltpu.VMEM((N_TP, PIECE, PIECE), BF16),
            pltpu.VMEM((N_TP, TOK, PIECE), BF16),
            pltpu.VMEM((4, TOK, PIECE), BF16),
            pltpu.VMEM((TOK, PIECE), BF16),
            pltpu.VMEM((2, TOK, PIECE), BF16),
            pltpu.VMEM((2, TOK // 2, PIECE), BF16),
            pltpu.VMEM((2, TOK, PIECE), BF16),
            pltpu.VMEM((TOK, PIECE), BF16),
            dma((N_TP,)),
            dma((28,)),
            dma((28,)),
        ],
        compiler_params=pltpu.CompilerParams(
            collective_id=0, has_side_effects=True, vmem_limit_bytes=63 * 2**20
        ),
        name="sublayer",
    )(
        hidden, norm_gain.reshape(1, WIDTH), freqs, doc_ids.reshape(1, TOK),
        w_query, w_key, w_value, w_out,
    )


def solution(mesh):
    in_specs = (
        P("cp", "tp"),
        P(),
        P(None, "tp"),
        P(None, "tp"),
        P(None, "tp"),
        P("tp", None),
        P("cp"),
    )
    return jax.shard_map(
        sublayer, mesh=mesh, in_specs=in_specs, out_specs=P("cp", "tp"), check_vma=False
    )
```

```python
import math

import jax
import jax.numpy as jnp
import numpy as np
from jax import lax
from jax.experimental import pallas as pl
from jax.experimental.pallas import tpu as pltpu
from jax.sharding import PartitionSpec as P

HEADS = 32
KV_HEADS = 8
HEAD_SIZE = 128
LONGEST = 12288
DOCS = 6
TOK = 512
GROUP = 4
ROWS = GROUP * TOK
BLK = 2 * TOK + 16
PENALTY = -(2.0**100)
SCALE = math.log2(math.e) / math.sqrt(HEAD_SIZE)
QC = 512

epsilon = 1e-05
rope_base = 500000.0


WIDTH = 4096
PIECE = 512
N_TP = 8
CH = 4
CR = TOK // CH
HALF = TOK // 2
MESH = pl.DeviceIdType.MESH


def tp_places():
    t = lax.axis_index("tp")
    plane = (t // 4) * 4
    y = t % 4
    up = plane + (y + 1) % 4
    down = plane + (y + 3) % 4
    far = plane + (y + 2) % 4
    return t, up, down, far


def other(t):
    return (t + 4) % 8


def part(chunk):
    return pl.ds(chunk * CR, CR)


def projection(
    h_ref, gain_ref, freq_ref, doc_ref, weights, inputs, q_out, kv_out, begin, serve,
    gath, w, acc, squares, cosine, sine, ssem, rsem, qssem, qrsem,
):
    t, up, down, far = tp_places()
    across = other(t)
    peers = [(t + i) % N_TP for i in range(1, N_TP)]
    for copy in inputs:
        copy.wait()
    sent = []

    def send(source, owner, chunk, to):
        copy = pltpu.make_async_remote_copy(
            src_ref=source,
            dst_ref=gath.at[owner, part(chunk)],
            send_sem=ssem.at[len(sent)],
            recv_sem=rsem.at[owner, chunk],
            device_id={"tp": to},
            device_id_type=MESH,
        )
        copy.start()
        sent.append(copy)

    def arrived(owner, chunk):
        pltpu.make_async_remote_copy(
            src_ref=gath.at[owner, part(chunk)],
            dst_ref=gath.at[owner, part(chunk)],
            send_sem=ssem.at[0],
            recv_sem=rsem.at[owner, chunk],
            device_id={"tp": across},
            device_id_type=MESH,
        ).wait_recv()

    def own(chunk, to):
        send(h_ref.at[part(chunk)], t, chunk, to)

    def relay(owner, chunk, to):
        send(gath.at[owner, part(chunk)], owner, chunk, to)

    own(0, up)
    own(1, down)
    own(0, across)
    mine = h_ref[...].astype(jnp.float32)
    mass = jnp.sum(mine * mine, axis=1, keepdims=True)
    squares[t] = jnp.broadcast_to(mass, (TOK, 128)).T[0:8]
    told = []
    for i, peer in enumerate(peers):
        copy = pltpu.make_async_remote_copy(
            src_ref=squares.at[t],
            dst_ref=squares.at[t],
            send_sem=qssem.at[i],
            recv_sem=qrsem.at[t],
            device_id={"tp": peer},
            device_id_type=MESH,
        )
        copy.start()
        told.append(copy)
    own(1, up)
    own(0, down)
    own(1, across)
    own(2, across)

    first = lax.axis_index("cp") * TOK
    place = (first + lax.broadcasted_iota(jnp.int32, (HEAD_SIZE // 2, TOK), 1)).astype(jnp.float32)
    angle = place * jnp.concatenate([freq_ref[...]] * (TOK // 128), axis=1)
    cosine[...] = jnp.cos(angle)
    sine[...] = jnp.sin(angle)
    for peer in peers:
        pltpu.make_async_remote_copy(
            src_ref=squares.at[peer],
            dst_ref=squares.at[peer],
            send_sem=qssem.at[0],
            recv_sem=qrsem.at[peer],
            device_id={"tp": peer},
            device_id_type=MESH,
        ).wait_recv()
    whole = jnp.sum(squares[...], axis=0)[0:1]
    inverse = lax.rsqrt(whole / WIDTH + epsilon)
    inverse = jnp.broadcast_to(inverse, (128, TOK)).T
    inverse = jnp.concatenate([inverse] * (PIECE // 128), axis=1)
    for copy in weights:
        copy.wait()

    def use(owner, second, start=False):
        rows = slice(second * HALF, (second + 1) * HALF)
        gain = gain_ref[:, pl.ds(pl.multiple_of(owner * PIECE, PIECE), PIECE)]
        wide = gath[owner, rows].astype(jnp.float32)
        normed = (wide * inverse[rows] * gain).astype(jnp.bfloat16)
        deep = pl.ds(pl.multiple_of(owner * PIECE, PIECE), PIECE)
        product = jnp.dot(normed, w[deep, :], preferred_element_type=jnp.float32)
        if start:
            acc[rows, :] = product
        else:
            acc[rows, :] += product

    half = HEAD_SIZE // 2

    def rotated(head, second):
        rows = slice(second * HALF, (second + 1) * HALF)
        raw = acc[rows, head * HEAD_SIZE : (head + 1) * HEAD_SIZE].T
        low = raw[:half] * cosine[:, rows] - raw[half:] * sine[:, rows]
        high = raw[half:] * cosine[:, rows] + raw[:half] * sine[:, rows]
        return low, high

    def finish_pairs(second):
        base = second * TOK
        rows = slice(second * HALF, (second + 1) * HALF)
        low, high = rotated(GROUP, second)
        turned = jnp.concatenate([low, high], axis=0).T
        kv_out[base : base + HALF, :] = turned.astype(jnp.bfloat16)
        value = acc[rows, (GROUP + 1) * HEAD_SIZE :].T.astype(jnp.bfloat16)
        for i in range(HALF // 128):
            at = base + HALF + 128 * i
            kv_out[at : at + 128, :] = value[:, 128 * i : 128 * (i + 1)]

    def finish_queries(second):
        for head in range(GROUP):
            low, high = rotated(head, second)
            cols = slice(head * TOK + second * HALF, head * TOK + (second + 1) * HALF)
            q_out[0:half, cols] = (low * SCALE).astype(jnp.bfloat16)
            q_out[half:HEAD_SIZE, cols] = (high * SCALE).astype(jnp.bfloat16)

    use(t, 0, True)
    arrived(down, 0)
    relay(down, 0, up)
    arrived(up, 1)
    relay(up, 1, down)
    for chunk in (0, 1):
        arrived(across, chunk)
        relay(across, chunk, up)
        relay(across, chunk, down)
    own(2, up)
    own(3, down)
    own(3, up)
    own(2, down)
    use(t, 1, True)
    lane = lax.broadcasted_iota(jnp.int32, (16, 128), 1)
    row = lax.broadcasted_iota(jnp.int32, (16, 128), 0)
    tail = jnp.zeros((16, 128), jnp.int32)
    for d in range(1, DOCS):
        count = jnp.sum(jnp.where(doc_ref[...] < d, 1, 0), axis=1, keepdims=True)
        tail = jnp.where(
            (lane == d) & (row == 0), count // 16, jnp.where((lane == d) & (row == 1), count % 16, tail)
        )
    kv_out[2 * TOK :, :] = tail.astype(jnp.float32).astype(jnp.bfloat16)
    arrived(down, 1)
    arrived(up, 0)
    use(up, 0)
    use(down, 0)
    arrived(far, 0)
    relay(far, 0, across)
    arrived(far, 1)
    relay(far, 1, across)
    own(3, across)
    use(across, 0)
    use(far, 0)
    for side in (up, down):
        arrived(other(side), 0)
        arrived(other(side), 1)
        use(other(side), 0)
    arrived(other(far), 0)
    arrived(other(far), 1)
    use(other(far), 0)
    finish_pairs(0)
    begin(0)
    arrived(down, 2)
    relay(down, 2, up)
    arrived(up, 3)
    relay(up, 3, down)
    for chunk in (2, 3):
        arrived(across, chunk)
        relay(across, chunk, up)
        relay(across, chunk, down)
    finish_queries(0)
    arrived(down, 3)
    arrived(up, 2)
    use(up, 1)
    use(down, 1)
    arrived(far, 2)
    relay(far, 2, across)
    arrived(far, 3)
    relay(far, 3, across)
    use(across, 1)
    for service in EARLY:
        serve(*service)
    use(far, 1)
    for side in (up, down):
        arrived(other(side), 2)
        arrived(other(side), 3)
        use(other(side), 1)
    arrived(other(far), 2)
    arrived(other(far), 3)
    use(other(far), 1)
    finish_pairs(1)
    begin(1)
    finish_queries(1)
    return sent + told


def combination(
    att, out_ref, weights, w, terms, sums, across_in, side_in, half_in, side_end, across_end, ssem, rsem,
):
    t, up, down, far = tp_places()
    across = other(t)
    sent = []

    def send(source, target, number, to):
        copy = pltpu.make_async_remote_copy(
            src_ref=source,
            dst_ref=target,
            send_sem=ssem.at[len(sent)],
            recv_sem=rsem.at[number],
            device_id={"tp": to},
            device_id_type=MESH,
        )
        copy.start()
        sent.append(copy)

    def arrived(target, number):
        pltpu.make_async_remote_copy(
            src_ref=target,
            dst_ref=target,
            send_sem=ssem.at[0],
            recv_sem=rsem.at[number],
            device_id={"tp": across},
            device_id_type=MESH,
        ).wait_recv()
        return target[...].astype(jnp.float32)

    def compute(i):
        weights[i].wait()
        product = jnp.dot(att[...], w[i], preferred_element_type=jnp.float32)
        terms[i] = product.astype(jnp.bfloat16)

    def term(i, chunk):
        return terms[i, part(chunk)].astype(jnp.float32)

    UP, DOWN = 0, 1
    compute(0)
    for chunk in (0, 2, 1, 3):
        send(terms.at[0, part(chunk)], across_in.at[part(chunk)], chunk, across)
    compute(1)
    compute(2)
    for chunk in range(CH):
        send(terms.at[1, part(chunk)], side_in.at[DOWN, part(chunk)], 4 + chunk, up)
        send(terms.at[2, part(chunk)], side_in.at[UP, part(chunk)], 8 + chunk, down)
    for i in range(3, 8):
        compute(i)
    for chunk in (0, 2, 1, 3):
        got = arrived(across_in.at[part(chunk)], chunk)
        sums[0, part(chunk)] = (term(3, chunk) + got).astype(jnp.bfloat16)
        if chunk < 2:
            send(sums.at[0, part(chunk)], half_in.at[DOWN, part(chunk)], 12 + chunk, up)
        else:
            send(sums.at[0, part(chunk)], half_in.at[UP, part(chunk - 2)], 12 + chunk, down)
    for chunk in range(CH):
        below = arrived(side_in.at[DOWN, part(chunk)], 4 + chunk)
        above = arrived(side_in.at[UP, part(chunk)], 8 + chunk)
        sums[1, part(chunk)] = (term(4, chunk) + below + above).astype(jnp.bfloat16)
        send(sums.at[1, part(chunk)], across_end.at[part(chunk)], 16 + chunk, across)
    for i in range(2):
        send(terms.at[5, part(2 + i)], side_end.at[DOWN, part(2 + i)], 22 + i, up)
        send(terms.at[6, part(i)], side_end.at[UP, part(i)], 24 + i, down)
    for i in range(2):
        got = arrived(half_in.at[DOWN, part(i)], 12 + i)
        sums[2, part(i)] = (term(5, i) + got).astype(jnp.bfloat16)
        send(sums.at[2, part(i)], side_end.at[DOWN, part(i)], 20 + i, up)
        got = arrived(half_in.at[UP, part(i)], 14 + i)
        sums[3, part(2 + i)] = (term(6, 2 + i) + got).astype(jnp.bfloat16)
        send(sums.at[3, part(2 + i)], side_end.at[UP, part(2 + i)], 26 + i, down)
    for chunk in range(CH):
        total = term(7, chunk) + arrived(across_end.at[part(chunk)], 16 + chunk)
        total = total + arrived(side_end.at[DOWN, part(chunk)], 20 + chunk)
        total = total + arrived(side_end.at[UP, part(chunk)], 24 + chunk)
        out_ref[part(chunk), :] = total.astype(jnp.bfloat16)
    return sent


def augment_queries(doc_ref, qaug):
    row = lax.broadcasted_iota(jnp.int32, (HEAD_SIZE, TOK), 0)
    hot = jnp.where(row == doc_ref[...], PENALTY, 0.0).astype(jnp.bfloat16)
    for head in range(GROUP):
        qaug[HEAD_SIZE:, head * TOK : (head + 1) * TOK] = hot


def attend_keys(block):
    counts = block[2 * TOK : 2 * TOK + 2, :].astype(jnp.float32)
    below = counts[0:1] * 16.0 + counts[1:2]
    row = lax.broadcasted_iota(jnp.int32, (TOK, HEAD_SIZE), 0).astype(jnp.float32)
    earlier = jnp.where(row < below, 1.0, 0.0).astype(jnp.bfloat16)
    keys = jnp.concatenate([block[0:HALF, :], block[TOK : TOK + HALF, :]], axis=0)
    return jnp.concatenate([keys, earlier], axis=1)


def score(keys, chunk, slot, qaug, logits, tops, causal):
    cols = slice(chunk * QC, (chunk + 1) * QC)
    length = keys.shape[0]
    scores = jnp.dot(keys, qaug[:, cols], preferred_element_type=jnp.float32)
    if causal:
        key_at = lax.broadcasted_iota(jnp.int32, (TOK, QC), 0)
        query_at = lax.broadcasted_iota(jnp.int32, (TOK, QC), 1) + (chunk * QC) % TOK
        scores = jnp.where(key_at <= query_at, scores, jnp.float32(PENALTY))
    logits[slot, 0:length] = scores
    tops[slot] = jnp.max(scores, axis=0, keepdims=True)


def weigh(values, chunk, slot, logits, tops, best, acc, first):
    cols = slice(chunk * QC, (chunk + 1) * QC)
    top = tops[slot]
    if not first:
        old = best[:, cols]
        top = jnp.maximum(old, top)
    weights = jnp.exp2(logits[slot, 0 : values.shape[1]] - top).astype(jnp.bfloat16)
    out = jnp.dot(values, weights, preferred_element_type=jnp.float32)
    if first:
        acc[:, cols] = out
    else:
        acc[:, cols] = acc[:, cols] * jnp.exp2(old - top) + out
    best[:, cols] = top


def attend(blocks, state, first):
    qaug, logits, tops, best, acc = state
    chunks = ROWS // QC
    keys = jnp.concatenate([attend_keys(block) for block in blocks], axis=0)
    values = jnp.concatenate(
        [
            block[at : at + 128, :]
            for block in blocks
            for at in (HALF, HALF + 128, TOK + HALF, TOK + HALF + 128)
        ],
        axis=1,
    )
    ones = jnp.ones((16, values.shape[1]), jnp.bfloat16)
    values = jnp.concatenate([values, ones], axis=0)
    score(keys, 0, 0, qaug, logits, tops, first)
    for chunk in range(chunks):
        if chunk + 1 < chunks:
            score(keys, chunk + 1, (chunk + 1) % 2, qaug, logits, tops, first)
        weigh(values, chunk, chunk % 2, logits, tops, best, acc, first)


def finish(acc, out_ref):
    for head in range(GROUP):
        cols = slice(head * TOK, (head + 1) * TOK)
        total = acc[HEAD_SIZE : HEAD_SIZE + 1, cols]
        out_ref[:, head * HEAD_SIZE : (head + 1) * HEAD_SIZE] = (
            (acc[0:HEAD_SIZE, cols] / total).T.astype(jnp.bfloat16)
        )


ROLES = 15
PARTS = ((0, TOK), (TOK, TOK + 16))
EARLY = [(0, 0), (2, 0), (15, 0), (3, 0), (4, 0), (1, 0)]
PROGRAM = [
    (0, [(5, 0), (6, 0), (11, 0), (7, 0), (0, 1), (15, 1)]),
    (2, [(2, 1), (9, 0)]),
    (1, [(3, 1), (4, 1), (1, 1), (12, 0), (13, 0)]),
    (3, [(8, 0), (10, 0)]),
    (4, [(5, 1), (6, 1), (14, 0)]),
    (5, [(11, 1), (7, 1)]),
    (6, [(9, 1)]),
    (9, [(8, 1)]),
    (8, []),
    (11, [(12, 1), (13, 1)]),
    (7, [(10, 1)]),
    (12, [(14, 1)]),
    (13, []),
    (10, []),
    (14, []),
]


def attention(
    doc_ref, own_ref, out_ref, kv, qaug, logits, tops, best, acc, ssem, rsem, sibsend, sibrecv,
):
    me = lax.axis_index("cp")
    core = me % 2
    x = (me // 2) % 4
    z = me // 8
    state = (qaug, logits, tops, best, acc)

    def at(zz, xx):
        return (zz * 4 + xx) * 2 + core

    right = at(z, (x + 1) % 4)
    left = at(z, (x + 3) % 4)
    ahead = at((z + 1) % 4, x)
    behind = at((z + 3) % 4, x)
    sibling = me + 1 - 2 * core

    def move(source, slot, half, to, send_sem, recv_sem):
        rows = pl.ds(*PARTS[half])
        return pltpu.make_async_remote_copy(
            src_ref=source.at[rows],
            dst_ref=kv.at[slot, rows],
            send_sem=send_sem,
            recv_sem=recv_sem,
            device_id={"cp": to},
            device_id_type=MESH,
        )

    always = z >= 0
    top = z == 3
    one, two = z >= 1, z >= 2
    xm, xp, x2 = (x + 3) % 4, (x + 1) % 4, (x + 2) % 4
    roles = [
        (x >= 1, z, xm),
        (x == 3, z, xp),
        (x >= 2, z, x2),
        (one, (z + 3) % 4, x),
        (top, 0 * z, x),
        (one, (z + 3) % 4, xm),
        (one, (z + 3) % 4, xp),
        (top & (x < 3), 0 * z, xp),
        (top & (x == 0), 0 * z, xm),
        (one, (z + 3) % 4, x2),
        (top & (x < 2), 0 * z, x2),
        (two, (z + 2) % 4, x),
        (two, (z + 2) % 4, xm),
        (two, (z + 2) % 4, xp),
        (two, (z + 2) % 4, x2),
        ((z == 0) & (x < 3), z, xp),
    ]
    slots = [at(zz, xx) for _, zz, xx in roles]
    middle = (x == 1) | (x == 2)
    forwards = {
        0: [(middle, right, (0, 1))],
        3: [(z < 3, ahead, (0, 1)), (always, right, (0, 1)), (always, left, (1, 0))],
        4: [(x == 3, right, (0, 1))],
        5: [(always, right, (0,))],
        6: [(always, left, (1,))],
        7: [(middle, left, (0, 1))],
        15: [(always, behind, (0, 1))],
        11: [(always, right, (0, 1)), (always, left, (1, 0))],
        12: [(always, right, (0,))],
        13: [(always, left, (1,))],
    }
    sends = []

    def plan(when, source, slot, half, to):
        number = len(sends)
        sends.append((when, source, slot, half, to))
        return number

    def issue(number):
        when, source, slot, half, to = sends[number]

        @pl.when(when)
        def _():
            move(source, slot, half, to, ssem.at[number], rsem.at[slot, half]).start()

    own = [[], []]
    for half in (0, 1):
        own[half].append(plan(z < 3, own_ref, me, half, ahead))
        own[half].append(plan(z == 0, own_ref, me, half, behind))
        own[half].append(plan(x < 3, own_ref, me, half, right))
        own[half].append(plan((x == 0) | (z == 0), own_ref, me, half, left))
    relays = {}
    for role, targets in forwards.items():
        relays[role] = {0: [], 1: []}
        for when, to, halves in targets:
            for half in halves:
                number = plan(roles[role][0] & when, kv.at[slots[role]], slots[role], half, to)
                relays[role][half].append(number)

    def begin(half):
        for number in own[half]:
            issue(number)
        move(own_ref, me, half, sibling, sibsend.at[ROLES, half], sibrecv.at[ROLES, half]).start()

    def serve(role, half):
        slot = slots[role]

        @pl.when(roles[role][0])
        def _():
            move(own_ref, slot, half, sibling, ssem.at[0], rsem.at[slot, half]).wait_recv()
            if role < ROLES:
                move(
                    kv.at[slot], slot, half, sibling, sibsend.at[role, half], sibrecv.at[role, half]
                ).start()

        for number in relays.get(role, {0: [], 1: []})[half]:
            issue(number)

    def run():
        augment_queries(doc_ref, qaug)
        attend([own_ref], state, True)
        for half in (0, 1):
            move(own_ref, sibling, half, sibling, sibsend.at[ROLES, half], sibrecv.at[ROLES, half]).wait_recv()

        @pl.when(core == 1)
        def _():
            attend([kv.at[sibling]], state, False)

        @pl.loop(0, ROLES)
        def _(step):
            there = step < 0
            slot = 0 * step
            turn = 0 * step
            for index, (role, services) in enumerate(PROGRAM):

                @pl.when(step == index)
                def _():
                    for service in services:
                        serve(*service)

                there = there | ((step == index) & roles[role][0])
                slot = jnp.where(step == index, slots[role], slot)
                turn = jnp.where(step == index, role, turn)

            @pl.when(there)
            def _():
                twin = slot + 1 - 2 * core
                for half in (0, 1):
                    move(own_ref, twin, half, sibling, sibsend.at[turn, half], sibrecv.at[turn, half]).wait_recv()
                attend([kv.at[slot], kv.at[twin]], state, False)

        finish(acc, out_ref)

    def drain():
        for number, (when, source, slot, half, to) in enumerate(sends):

            @pl.when(when)
            def _():
                move(source, slot, half, to, ssem.at[number], rsem.at[slot, half]).wait_send()

        for role in range(ROLES + 1):
            present, slot = (always, me) if role == ROLES else (roles[role][0], slots[role])
            for half in (0, 1):

                @pl.when(present)
                def _():
                    move(
                        own_ref, slot, half, sibling, sibsend.at[role, half], sibrecv.at[role, half]
                    ).wait_send()

    return begin, serve, run, drain


SENDS = 30
BF16, F32 = jnp.bfloat16, jnp.float32


def fused_kernel(
    h_hbm, gain_hbm, freq_hbm, doc_hbm, wq, wk, wv, w_out, out_ref,
    gath, w, pacc, squares, cosine, sine, gain_ref, freq_ref, doc_ref, insem, pssem, prsem, qssem, qrsem,
    own, kv, qaug, logits, tops, best, acc, assem, arsem, sibsend, sibrecv, att,
    wo, terms, sums, across_in, side_in, half_in, side_end, across_end, wosem, cssem, crsem,
):
    t, up, down, far = tp_places()
    across = other(t)
    me = lax.axis_index("cp")
    h_ref = gath.at[t]
    inputs = [
        pltpu.make_async_copy(h_hbm, h_ref, insem.at[0]),
        pltpu.make_async_copy(freq_hbm, freq_ref, insem.at[1]),
        pltpu.make_async_copy(gain_hbm, gain_ref, insem.at[2]),
        pltpu.make_async_copy(doc_hbm, doc_ref, insem.at[3]),
    ]
    weights = [
        pltpu.make_async_copy(wq, w.at[:, 0:512], insem.at[4]),
        pltpu.make_async_copy(wk, w.at[:, 512:640], insem.at[5]),
        pltpu.make_async_copy(wv, w.at[:, 640:768], insem.at[6]),
    ]
    order = [other(far), other(up), other(down), far, across, up, down, t]
    late = []
    for i, owner in enumerate(order):
        cols = pl.ds(pl.multiple_of(owner * PIECE, PIECE), PIECE)
        late.append(pltpu.make_async_copy(w_out.at[:, cols], wo.at[i], wosem.at[i]))
    for copy in inputs + weights + late:
        copy.start()
    core = me % 2
    column = (me // 2) % 4
    row = me // 8
    barrier = pltpu.get_barrier_semaphore()
    around = [
        me - me % 8 + (me + 2) % 8,
        me - me % 8 + (me + 6) % 8,
        (me + 8) % 32,
        (me + 24) % 32,
        me + 1 - 2 * core,
    ]
    for i in range(1, N_TP):
        pl.semaphore_signal(barrier, inc=1, device_id={"tp": (t + i) % N_TP}, device_id_type=MESH)
    for peer in around:
        pl.semaphore_signal(barrier, inc=1, device_id={"cp": peer}, device_id_type=MESH)
    pl.semaphore_wait(barrier, N_TP - 1 + len(around))

    begin, serve, run, drain = attention(
        doc_ref, own, att, kv, qaug, logits, tops, best, acc, assem, arsem, sibsend, sibrecv
    )
    sent = projection(
        h_ref, gain_ref, freq_ref, doc_ref, weights, inputs, qaug, own, begin, serve,
        gath, w, pacc, squares, cosine, sine, pssem, prsem, qssem, qrsem,
    )
    run()
    sent += combination(
        att, out_ref, late, wo, terms, sums, across_in, side_in, half_in, side_end, across_end, cssem, crsem
    )
    drain()
    for copy in sent:
        copy.wait_send()


def sublayer(hidden, norm_gain, w_query, w_key, w_value, w_out, doc_ids):
    hbm = pl.BlockSpec(memory_space=pl.ANY)
    powers = -np.arange(HEAD_SIZE // 2, dtype=np.float32) * np.float32(2.0) / HEAD_SIZE
    freqs = (np.float64(rope_base) ** powers.astype(np.float64)).astype(np.float32)
    freqs = jnp.asarray(np.broadcast_to(freqs[:, None], (HEAD_SIZE // 2, 128)))
    dma = pltpu.SemaphoreType.DMA
    return pl.pallas_call(
        fused_kernel,
        out_shape=jax.ShapeDtypeStruct((TOK, PIECE), BF16),
        in_specs=[hbm] * 8,
        out_specs=pl.BlockSpec(memory_space=pltpu.VMEM),
        scratch_shapes=[
            pltpu.VMEM((N_TP, TOK, PIECE), BF16),
            pltpu.VMEM((WIDTH, 768), BF16),
            pltpu.VMEM((TOK, 768), F32),
            pltpu.VMEM((N_TP, 8, TOK), F32),
            pltpu.VMEM((HEAD_SIZE // 2, TOK), F32),
            pltpu.VMEM((HEAD_SIZE // 2, TOK), F32),
            pltpu.VMEM((1, WIDTH), F32),
            pltpu.VMEM((HEAD_SIZE // 2, 128), F32),
            pltpu.VMEM((1, TOK), jnp.int32),
            dma((7,)),
            dma((28,)),
            dma((N_TP, CH)),
            dma((N_TP - 1,)),
            dma((N_TP,)),
            pltpu.VMEM((BLK, 128), BF16),
            pltpu.VMEM((32, BLK, 128), BF16),
            pltpu.VMEM((2 * HEAD_SIZE, ROWS), BF16),
            pltpu.VMEM((2, 2 * TOK, QC), F32),
            pltpu.VMEM((2, 1, QC), F32),
            pltpu.VMEM((1, ROWS), F32),
            pltpu.VMEM((HEAD_SIZE + 16, ROWS), F32),
            dma((SENDS,)),
            dma((32, 2)),
            dma((ROLES + 1, 2)),
            dma((ROLES + 1, 2)),
            pltpu.VMEM((TOK, GROUP * HEAD_SIZE), BF16),
            pltpu.VMEM((N_TP, PIECE, PIECE), BF16),
            pltpu.VMEM((N_TP, TOK, PIECE), BF16),
            pltpu.VMEM((4, TOK, PIECE), BF16),
            pltpu.VMEM((TOK, PIECE), BF16),
            pltpu.VMEM((2, TOK, PIECE), BF16),
            pltpu.VMEM((2, TOK // 2, PIECE), BF16),
            pltpu.VMEM((2, TOK, PIECE), BF16),
            pltpu.VMEM((TOK, PIECE), BF16),
            dma((N_TP,)),
            dma((28,)),
            dma((28,)),
        ],
        compiler_params=pltpu.CompilerParams(
            collective_id=0, has_side_effects=True, vmem_limit_bytes=63 * 2**20
        ),
        name="sublayer",
    )(
        hidden, norm_gain.reshape(1, WIDTH), freqs, doc_ids.reshape(1, TOK),
        w_query, w_key, w_value, w_out,
    )


def solution(mesh):
    in_specs = (
        P("cp", "tp"),
        P(),
        P(None, "tp"),
        P(None, "tp"),
        P(None, "tp"),
        P("tp", None),
        P("cp"),
    )
    return jax.shard_map(
        sublayer, mesh=mesh, in_specs=in_specs, out_specs=P("cp", "tp"), check_vma=False
    )
```

```python
import math

import jax
import jax.numpy as jnp
from jax import lax
from jax.experimental import pallas as pl
from jax.experimental.pallas import tpu as pltpu
from jax.sharding import PartitionSpec as P

HEADS = 32
KV_HEADS = 8
HEAD_SIZE = 128
LONGEST = 12288
DOCS = 6
TOK = 512
GROUP = 4
ROWS = GROUP * TOK
BLK = 2 * TOK + 16
PENALTY = -(2.0**100)
SCALE = math.log2(math.e) / math.sqrt(HEAD_SIZE)
QC = 512

epsilon = 1e-05
rope_base = 500000.0


WIDTH = 4096
PIECE = 512
N_TP = 8
CH = 4
CR = TOK // CH
MESH = pl.DeviceIdType.MESH


def tp_places():
    t = lax.axis_index("tp")
    plane = (t // 4) * 4
    y = t % 4
    up = plane + (y + 1) % 4
    down = plane + (y + 3) % 4
    far = plane + (y + 2) % 4
    return t, up, down, far


def other(t):
    return (t + 4) % 8


def part(chunk):
    return pl.ds(chunk * CR, CR)


def projection(
    h_ref, gain_ref, doc_ref, weights, inputs, q_out, kv_out, begin,
    gath, w, acc, squares, cosine, sine, ssem, rsem, qssem, qrsem,
):
    t, up, down, far = tp_places()
    across = other(t)
    peers = [(t + i) % N_TP for i in range(1, N_TP)]
    for copy in inputs:
        copy.wait()
    sent = []

    def send(source, owner, chunk, to):
        copy = pltpu.make_async_remote_copy(
            src_ref=source,
            dst_ref=gath.at[owner, part(chunk)],
            send_sem=ssem.at[len(sent)],
            recv_sem=rsem.at[owner, chunk],
            device_id={"tp": to},
            device_id_type=MESH,
        )
        copy.start()
        sent.append(copy)

    def arrived(owner, chunk):
        pltpu.make_async_remote_copy(
            src_ref=gath.at[owner, part(chunk)],
            dst_ref=gath.at[owner, part(chunk)],
            send_sem=ssem.at[0],
            recv_sem=rsem.at[owner, chunk],
            device_id={"tp": across},
            device_id_type=MESH,
        ).wait_recv()

    upward = (0, 1, 2, 3)
    downward = (2, 3, 0, 1)

    def send_own(i):
        send(h_ref.at[part(upward[i])], t, upward[i], up)
        send(h_ref.at[part(downward[i])], t, downward[i], down)
        send(h_ref.at[part(upward[i])], t, upward[i], across)

    send_own(0)
    mine = h_ref[...].astype(jnp.float32)
    mass = jnp.sum(mine * mine, axis=1, keepdims=True)
    squares[t] = jnp.broadcast_to(mass, (TOK, 128)).T[0:8]
    told = []
    for i, peer in enumerate(peers):
        copy = pltpu.make_async_remote_copy(
            src_ref=squares.at[t],
            dst_ref=squares.at[t],
            send_sem=qssem.at[i],
            recv_sem=qrsem.at[t],
            device_id={"tp": peer},
            device_id_type=MESH,
        )
        copy.start()
        told.append(copy)
    for i in range(1, CH):
        send_own(i)

    first = lax.axis_index("cp") * TOK
    place = (first + lax.broadcasted_iota(jnp.int32, (HEAD_SIZE // 2, TOK), 1)).astype(jnp.float32)
    pair = lax.broadcasted_iota(jnp.int32, (HEAD_SIZE // 2, 128), 0)
    freqs = jnp.zeros((HEAD_SIZE // 2, 128), jnp.float32)
    for i in range(HEAD_SIZE // 2):
        freqs = jnp.where(pair == i, jnp.float32(rope_base ** (-2.0 * i / HEAD_SIZE)), freqs)
    angle = place * jnp.concatenate([freqs] * (TOK // 128), axis=1)
    cosine[...] = jnp.cos(angle)
    sine[...] = jnp.sin(angle)
    for peer in peers:
        pltpu.make_async_remote_copy(
            src_ref=squares.at[peer],
            dst_ref=squares.at[peer],
            send_sem=qssem.at[0],
            recv_sem=qrsem.at[peer],
            device_id={"tp": peer},
            device_id_type=MESH,
        ).wait_recv()
    whole = jnp.sum(squares[...], axis=0)[0:1]
    inverse = lax.rsqrt(whole / WIDTH + epsilon)
    inverse = jnp.broadcast_to(inverse, (128, TOK)).T
    inverse = jnp.concatenate([inverse] * (PIECE // 128), axis=1)
    for copy in weights:
        copy.wait()

    def use(source, owner, start):
        gain = gain_ref[:, pl.ds(pl.multiple_of(owner * PIECE, PIECE), PIECE)]
        normed = (source[...].astype(jnp.float32) * inverse * gain).astype(jnp.bfloat16)
        rows = pl.ds(pl.multiple_of(owner * PIECE, PIECE), PIECE)
        product = jnp.dot(normed, w[rows, :], preferred_element_type=jnp.float32)
        if start:
            acc[...] = product
        else:
            acc[...] += product

    use(h_ref, t, True)
    for i in range(CH):
        arrived(down, upward[i])
        if i < 2:
            send(gath.at[down, part(upward[i])], down, upward[i], up)
        arrived(up, downward[i])
        if i < 2:
            send(gath.at[up, part(downward[i])], up, downward[i], down)
        arrived(across, upward[i])
        if i == 1:
            for chunk in (0, 1):
                send(gath.at[across, part(chunk)], across, chunk, up)
                send(gath.at[across, part(chunk)], across, chunk, down)
        if i > 1:
            send(gath.at[across, part(i)], across, i, up)
            send(gath.at[across, part(i)], across, i, down)
    use(gath.at[up], up, False)
    use(gath.at[down], down, False)
    for i in range(2):
        for chunk in (upward[i], downward[i]):
            arrived(far, chunk)
            send(gath.at[far, part(chunk)], far, chunk, across)
    use(gath.at[across], across, False)
    use(gath.at[far], far, False)
    for chunk in (0, 2, 1, 3):
        arrived(other(far), chunk)
    use(gath.at[other(far)], other(far), False)
    for side in (up, down):
        for chunk in range(CH):
            arrived(other(side), chunk)
        use(gath.at[other(side)], other(side), False)

    half = HEAD_SIZE // 2

    def rotated(head):
        raw = acc[:, head * HEAD_SIZE : (head + 1) * HEAD_SIZE].T
        low = raw[:half] * cosine[...] - raw[half:] * sine[...]
        high = raw[half:] * cosine[...] + raw[:half] * sine[...]
        return low, high

    low, high = rotated(GROUP)
    kv_out[0:TOK, :] = jnp.concatenate([low, high], axis=0).T.astype(jnp.bfloat16)
    value = acc[:, (GROUP + 1) * HEAD_SIZE :].T.astype(jnp.bfloat16)
    for i in range(TOK // 128):
        kv_out[TOK + 128 * i : TOK + 128 * (i + 1), :] = value[:, 128 * i : 128 * (i + 1)]
    lane = lax.broadcasted_iota(jnp.int32, (16, 128), 1)
    row = lax.broadcasted_iota(jnp.int32, (16, 128), 0)
    tail = jnp.zeros((16, 128), jnp.int32)
    for d in range(1, DOCS):
        count = jnp.sum(jnp.where(doc_ref[...] < d, 1, 0), axis=1, keepdims=True)
        tail = jnp.where(
            (lane == d) & (row == 0), count // 16, jnp.where((lane == d) & (row == 1), count % 16, tail)
        )
    kv_out[2 * TOK :, :] = tail.astype(jnp.float32).astype(jnp.bfloat16)
    begin()
    for head in range(GROUP):
        low, high = rotated(head)
        cols = slice(head * TOK, (head + 1) * TOK)
        q_out[0:half, cols] = (low * SCALE).astype(jnp.bfloat16)
        q_out[half:HEAD_SIZE, cols] = (high * SCALE).astype(jnp.bfloat16)
    return sent + told


def combination(
    att, out_ref, weights, w, terms, sums, across_in, side_in, half_in, side_end, across_end, ssem, rsem,
):
    t, up, down, far = tp_places()
    across = other(t)
    sent = []

    def send(source, target, number, to):
        copy = pltpu.make_async_remote_copy(
            src_ref=source,
            dst_ref=target,
            send_sem=ssem.at[len(sent)],
            recv_sem=rsem.at[number],
            device_id={"tp": to},
            device_id_type=MESH,
        )
        copy.start()
        sent.append(copy)

    def arrived(target, number):
        pltpu.make_async_remote_copy(
            src_ref=target,
            dst_ref=target,
            send_sem=ssem.at[0],
            recv_sem=rsem.at[number],
            device_id={"tp": across},
            device_id_type=MESH,
        ).wait_recv()
        return target[...].astype(jnp.float32)

    def compute(i):
        weights[i].wait()
        product = jnp.dot(att[...], w[i], preferred_element_type=jnp.float32)
        terms[i] = product.astype(jnp.bfloat16)

    def term(i, chunk):
        return terms[i, part(chunk)].astype(jnp.float32)

    UP, DOWN = 0, 1
    compute(0)
    for chunk in (0, 2, 1, 3):
        send(terms.at[0, part(chunk)], across_in.at[part(chunk)], chunk, across)
    compute(1)
    compute(2)
    for chunk in range(CH):
        send(terms.at[1, part(chunk)], side_in.at[DOWN, part(chunk)], 4 + chunk, up)
        send(terms.at[2, part(chunk)], side_in.at[UP, part(chunk)], 8 + chunk, down)
    for i in range(3, 8):
        compute(i)
    for chunk in (0, 2, 1, 3):
        got = arrived(across_in.at[part(chunk)], chunk)
        sums[0, part(chunk)] = (term(3, chunk) + got).astype(jnp.bfloat16)
        if chunk < 2:
            send(sums.at[0, part(chunk)], half_in.at[DOWN, part(chunk)], 12 + chunk, up)
        else:
            send(sums.at[0, part(chunk)], half_in.at[UP, part(chunk - 2)], 12 + chunk, down)
    for chunk in range(CH):
        below = arrived(side_in.at[DOWN, part(chunk)], 4 + chunk)
        above = arrived(side_in.at[UP, part(chunk)], 8 + chunk)
        sums[1, part(chunk)] = (term(4, chunk) + below + above).astype(jnp.bfloat16)
        send(sums.at[1, part(chunk)], across_end.at[part(chunk)], 16 + chunk, across)
    for i in range(2):
        send(terms.at[5, part(2 + i)], side_end.at[DOWN, part(2 + i)], 22 + i, up)
        send(terms.at[6, part(i)], side_end.at[UP, part(i)], 24 + i, down)
    for i in range(2):
        got = arrived(half_in.at[DOWN, part(i)], 12 + i)
        sums[2, part(i)] = (term(5, i) + got).astype(jnp.bfloat16)
        send(sums.at[2, part(i)], side_end.at[DOWN, part(i)], 20 + i, up)
        got = arrived(half_in.at[UP, part(i)], 14 + i)
        sums[3, part(2 + i)] = (term(6, 2 + i) + got).astype(jnp.bfloat16)
        send(sums.at[3, part(2 + i)], side_end.at[UP, part(2 + i)], 26 + i, down)
    for chunk in range(CH):
        total = term(7, chunk) + arrived(across_end.at[part(chunk)], 16 + chunk)
        total = total + arrived(side_end.at[DOWN, part(chunk)], 20 + chunk)
        total = total + arrived(side_end.at[UP, part(chunk)], 24 + chunk)
        out_ref[part(chunk), :] = total.astype(jnp.bfloat16)
    return sent


def augment_queries(doc_ref, qaug):
    row = lax.broadcasted_iota(jnp.int32, (HEAD_SIZE, TOK), 0)
    hot = jnp.where(row == doc_ref[...], PENALTY, 0.0).astype(jnp.bfloat16)
    for head in range(GROUP):
        qaug[HEAD_SIZE:, head * TOK : (head + 1) * TOK] = hot


def attend_keys(block):
    counts = block[2 * TOK : 2 * TOK + 2, :].astype(jnp.float32)
    below = counts[0:1] * 16.0 + counts[1:2]
    row = lax.broadcasted_iota(jnp.int32, (TOK, HEAD_SIZE), 0).astype(jnp.float32)
    earlier = jnp.where(row < below, 1.0, 0.0).astype(jnp.bfloat16)
    return jnp.concatenate([block[0:TOK, :], earlier], axis=1)


def score(keys, chunk, slot, qaug, logits, tops, causal):
    cols = slice(chunk * QC, (chunk + 1) * QC)
    length = keys.shape[0]
    scores = jnp.dot(keys, qaug[:, cols], preferred_element_type=jnp.float32)
    if causal:
        key_at = lax.broadcasted_iota(jnp.int32, (TOK, QC), 0)
        query_at = lax.broadcasted_iota(jnp.int32, (TOK, QC), 1) + (chunk * QC) % TOK
        scores = jnp.where(key_at <= query_at, scores, jnp.float32(PENALTY))
    logits[slot, 0:length] = scores
    tops[slot] = jnp.max(scores, axis=0, keepdims=True)


def weigh(values, chunk, slot, logits, tops, best, acc, first):
    cols = slice(chunk * QC, (chunk + 1) * QC)
    top = tops[slot]
    if not first:
        old = best[:, cols]
        top = jnp.maximum(old, top)
    weights = jnp.exp2(logits[slot, 0 : values.shape[1]] - top).astype(jnp.bfloat16)
    out = jnp.dot(values, weights, preferred_element_type=jnp.float32)
    if first:
        acc[:, cols] = out
    else:
        acc[:, cols] = acc[:, cols] * jnp.exp2(old - top) + out
    best[:, cols] = top


def attend(blocks, state, first):
    qaug, logits, tops, best, acc = state
    chunks = ROWS // QC
    keys = jnp.concatenate([attend_keys(block) for block in blocks], axis=0)
    values = jnp.concatenate(
        [
            block[TOK + 128 * i : TOK + 128 * (i + 1), :]
            for block in blocks
            for i in range(TOK // 128)
        ],
        axis=1,
    )
    ones = jnp.ones((16, values.shape[1]), jnp.bfloat16)
    values = jnp.concatenate([values, ones], axis=0)
    score(keys, 0, 0, qaug, logits, tops, first)
    for chunk in range(chunks):
        if chunk + 1 < chunks:
            score(keys, chunk + 1, (chunk + 1) % 2, qaug, logits, tops, first)
        weigh(values, chunk, chunk % 2, logits, tops, best, acc, first)


def finish(acc, out_ref):
    for head in range(GROUP):
        cols = slice(head * TOK, (head + 1) * TOK)
        total = acc[HEAD_SIZE : HEAD_SIZE + 1, cols]
        out_ref[:, head * HEAD_SIZE : (head + 1) * HEAD_SIZE] = (
            (acc[0:HEAD_SIZE, cols] / total).T.astype(jnp.bfloat16)
        )


ROLES = 15
PARTS = ((0, TOK), (TOK, TOK + 16))
PROGRAM = [
    (0, [(0, 0), (0, 1), (15, 0), (15, 1)]),
    (2, [(2, 0), (2, 1), (3, 0), (4, 0)]),
    (1, [(1, 0), (1, 1), (3, 1), (4, 1)]),
    (3, []),
    (4, [(5, 0), (6, 0)]),
    (5, [(5, 1), (6, 1)]),
    (6, [(11, 0), (7, 0)]),
    (9, [(9, 0), (9, 1)]),
    (8, [(8, 0), (8, 1)]),
    (11, [(11, 1), (12, 0), (13, 0), (7, 1)]),
    (7, []),
    (12, [(12, 1), (13, 1)]),
    (13, [(10, 0), (10, 1)]),
    (10, [(14, 0), (14, 1)]),
    (14, []),
]


def attention(
    doc_ref, own_ref, out_ref, kv, qaug, logits, tops, best, acc, ssem, rsem, sibsend, sibrecv,
):
    me = lax.axis_index("cp")
    core = me % 2
    x = (me // 2) % 4
    z = me // 8
    state = (qaug, logits, tops, best, acc)

    def at(zz, xx):
        return (zz * 4 + xx) * 2 + core

    right = at(z, (x + 1) % 4)
    left = at(z, (x + 3) % 4)
    ahead = at((z + 1) % 4, x)
    behind = at((z + 3) % 4, x)
    sibling = me + 1 - 2 * core

    def move(source, slot, half, to, send_sem, recv_sem):
        rows = pl.ds(*PARTS[half])
        return pltpu.make_async_remote_copy(
            src_ref=source.at[rows],
            dst_ref=kv.at[slot, rows],
            send_sem=send_sem,
            recv_sem=recv_sem,
            device_id={"cp": to},
            device_id_type=MESH,
        )

    always = z >= 0
    top = z == 3
    one, two = z >= 1, z >= 2
    xm, xp, x2 = (x + 3) % 4, (x + 1) % 4, (x + 2) % 4
    roles = [
        (x >= 1, z, xm),
        (x == 3, z, xp),
        (x >= 2, z, x2),
        (one, (z + 3) % 4, x),
        (top, 0 * z, x),
        (one, (z + 3) % 4, xm),
        (one, (z + 3) % 4, xp),
        (top & (x < 3), 0 * z, xp),
        (top & (x == 0), 0 * z, xm),
        (one, (z + 3) % 4, x2),
        (top & (x < 2), 0 * z, x2),
        (two, (z + 2) % 4, x),
        (two, (z + 2) % 4, xm),
        (two, (z + 2) % 4, xp),
        (two, (z + 2) % 4, x2),
        ((z == 0) & (x < 3), z, xp),
    ]
    slots = [at(zz, xx) for _, zz, xx in roles]
    middle = (x == 1) | (x == 2)
    forwards = {
        0: [(middle, right, (0, 1))],
        3: [(z < 3, ahead, (0, 1)), (always, right, (0, 1)), (always, left, (1, 0))],
        4: [(x == 3, right, (0, 1))],
        5: [(always, right, (0,))],
        6: [(always, left, (1,))],
        7: [(middle, left, (0, 1))],
        15: [(always, behind, (0, 1))],
        11: [(always, right, (0, 1)), (always, left, (1, 0))],
        12: [(always, right, (0,))],
        13: [(always, left, (1,))],
    }
    sends = []

    def plan(when, source, slot, half, to):
        number = len(sends)
        sends.append((when, source, slot, half, to))
        return number

    def issue(number):
        when, source, slot, half, to = sends[number]

        @pl.when(when)
        def _():
            move(source, slot, half, to, ssem.at[number], rsem.at[slot, half]).start()

    own = []
    for half in (0, 1):
        own.append(plan(z < 3, own_ref, me, half, ahead))
        own.append(plan(z == 0, own_ref, me, half, behind))
        own.append(plan(x < 3, own_ref, me, half, right))
        own.append(plan((x == 0) | (z == 0), own_ref, me, half, left))
    relays = {}
    for role, targets in forwards.items():
        relays[role] = {0: [], 1: []}
        for when, to, halves in targets:
            for half in halves:
                number = plan(roles[role][0] & when, kv.at[slots[role]], slots[role], half, to)
                relays[role][half].append(number)

    def begin():
        for number in own:
            issue(number)
        for half in (0, 1):
            move(own_ref, me, half, sibling, sibsend.at[ROLES, half], sibrecv.at[ROLES, half]).start()

    def serve(role, half):
        slot = slots[role]

        @pl.when(roles[role][0])
        def _():
            move(own_ref, slot, half, sibling, ssem.at[0], rsem.at[slot, half]).wait_recv()
            if role < ROLES:
                move(
                    kv.at[slot], slot, half, sibling, sibsend.at[role, half], sibrecv.at[role, half]
                ).start()

        for number in relays.get(role, {0: [], 1: []})[half]:
            issue(number)

    def run():
        augment_queries(doc_ref, qaug)
        attend([own_ref], state, True)
        for half in (0, 1):
            move(own_ref, sibling, half, sibling, sibsend.at[ROLES, half], sibrecv.at[ROLES, half]).wait_recv()

        @pl.when(core == 1)
        def _():
            attend([kv.at[sibling]], state, False)

        @pl.loop(0, ROLES)
        def _(step):
            there = step < 0
            slot = 0 * step
            turn = 0 * step
            for index, (role, services) in enumerate(PROGRAM):

                @pl.when(step == index)
                def _():
                    for service in services:
                        serve(*service)

                there = there | ((step == index) & roles[role][0])
                slot = jnp.where(step == index, slots[role], slot)
                turn = jnp.where(step == index, role, turn)

            @pl.when(there)
            def _():
                twin = slot + 1 - 2 * core
                for half in (0, 1):
                    move(own_ref, twin, half, sibling, sibsend.at[turn, half], sibrecv.at[turn, half]).wait_recv()
                attend([kv.at[slot], kv.at[twin]], state, False)

        finish(acc, out_ref)

    def drain():
        for number, (when, source, slot, half, to) in enumerate(sends):

            @pl.when(when)
            def _():
                move(source, slot, half, to, ssem.at[number], rsem.at[slot, half]).wait_send()

        for role in range(ROLES + 1):
            present, slot = (always, me) if role == ROLES else (roles[role][0], slots[role])
            for half in (0, 1):

                @pl.when(present)
                def _():
                    move(
                        own_ref, slot, half, sibling, sibsend.at[role, half], sibrecv.at[role, half]
                    ).wait_send()

    return begin, run, drain


SENDS = 30
BF16, F32 = jnp.bfloat16, jnp.float32


def fused_kernel(
    h_hbm, gain_hbm, doc_hbm, wq, wk, wv, w_out, out_ref,
    gath, w, pacc, squares, cosine, sine, gain_ref, doc_ref, insem, pssem, prsem, qssem, qrsem,
    own, kv, qaug, logits, tops, best, acc, assem, arsem, sibsend, sibrecv, att,
    wo, terms, sums, across_in, side_in, half_in, side_end, across_end, wosem, cssem, crsem,
):
    t, up, down, far = tp_places()
    across = other(t)
    me = lax.axis_index("cp")
    h_ref = gath.at[t]
    inputs = [
        pltpu.make_async_copy(h_hbm, h_ref, insem.at[0]),
        pltpu.make_async_copy(gain_hbm, gain_ref, insem.at[1]),
        pltpu.make_async_copy(doc_hbm, doc_ref, insem.at[2]),
    ]
    weights = [
        pltpu.make_async_copy(wq, w.at[:, 0:512], insem.at[3]),
        pltpu.make_async_copy(wk, w.at[:, 512:640], insem.at[4]),
        pltpu.make_async_copy(wv, w.at[:, 640:768], insem.at[5]),
    ]
    order = [other(far), other(up), other(down), far, across, up, down, t]
    late = []
    for i, owner in enumerate(order):
        cols = pl.ds(pl.multiple_of(owner * PIECE, PIECE), PIECE)
        late.append(pltpu.make_async_copy(w_out.at[:, cols], wo.at[i], wosem.at[i]))
    for copy in inputs + weights + late:
        copy.start()
    core = me % 2
    column = (me // 2) % 4
    row = me // 8
    barrier = pltpu.get_barrier_semaphore()
    around = [
        me - me % 8 + (me + 2) % 8,
        me - me % 8 + (me + 6) % 8,
        (me + 8) % 32,
        (me + 24) % 32,
        me + 1 - 2 * core,
    ]
    for i in range(1, N_TP):
        pl.semaphore_signal(barrier, inc=1, device_id={"tp": (t + i) % N_TP}, device_id_type=MESH)
    for peer in around:
        pl.semaphore_signal(barrier, inc=1, device_id={"cp": peer}, device_id_type=MESH)
    pl.semaphore_wait(barrier, N_TP - 1 + len(around))

    begin, run, drain = attention(
        doc_ref, own, att, kv, qaug, logits, tops, best, acc, assem, arsem, sibsend, sibrecv
    )
    sent = projection(
        h_ref, gain_ref, doc_ref, weights, inputs, qaug, own, begin,
        gath, w, pacc, squares, cosine, sine, pssem, prsem, qssem, qrsem,
    )
    run()
    sent += combination(
        att, out_ref, late, wo, terms, sums, across_in, side_in, half_in, side_end, across_end, cssem, crsem
    )
    drain()
    for copy in sent:
        copy.wait_send()


def sublayer(hidden, norm_gain, w_query, w_key, w_value, w_out, doc_ids):
    hbm = pl.BlockSpec(memory_space=pl.ANY)
    dma = pltpu.SemaphoreType.DMA
    return pl.pallas_call(
        fused_kernel,
        out_shape=jax.ShapeDtypeStruct((TOK, PIECE), BF16),
        in_specs=[hbm] * 7,
        out_specs=pl.BlockSpec(memory_space=pltpu.VMEM),
        scratch_shapes=[
            pltpu.VMEM((N_TP, TOK, PIECE), BF16),
            pltpu.VMEM((WIDTH, 768), BF16),
            pltpu.VMEM((TOK, 768), F32),
            pltpu.VMEM((N_TP, 8, TOK), F32),
            pltpu.VMEM((HEAD_SIZE // 2, TOK), F32),
            pltpu.VMEM((HEAD_SIZE // 2, TOK), F32),
            pltpu.VMEM((1, WIDTH), F32),
            pltpu.VMEM((1, TOK), jnp.int32),
            dma((6,)),
            dma((28,)),
            dma((N_TP, CH)),
            dma((N_TP - 1,)),
            dma((N_TP,)),
            pltpu.VMEM((BLK, 128), BF16),
            pltpu.VMEM((32, BLK, 128), BF16),
            pltpu.VMEM((2 * HEAD_SIZE, ROWS), BF16),
            pltpu.VMEM((2, 2 * TOK, QC), F32),
            pltpu.VMEM((2, 1, QC), F32),
            pltpu.VMEM((1, ROWS), F32),
            pltpu.VMEM((HEAD_SIZE + 16, ROWS), F32),
            dma((SENDS,)),
            dma((32, 2)),
            dma((ROLES + 1, 2)),
            dma((ROLES + 1, 2)),
            pltpu.VMEM((TOK, GROUP * HEAD_SIZE), BF16),
            pltpu.VMEM((N_TP, PIECE, PIECE), BF16),
            pltpu.VMEM((N_TP, TOK, PIECE), BF16),
            pltpu.VMEM((4, TOK, PIECE), BF16),
            pltpu.VMEM((TOK, PIECE), BF16),
            pltpu.VMEM((2, TOK, PIECE), BF16),
            pltpu.VMEM((2, TOK // 2, PIECE), BF16),
            pltpu.VMEM((2, TOK, PIECE), BF16),
            pltpu.VMEM((TOK, PIECE), BF16),
            dma((N_TP,)),
            dma((28,)),
            dma((28,)),
        ],
        compiler_params=pltpu.CompilerParams(
            collective_id=0, has_side_effects=True, vmem_limit_bytes=63 * 2**20
        ),
        name="sublayer",
    )(
        hidden, norm_gain.reshape(1, WIDTH), doc_ids.reshape(1, TOK),
        w_query, w_key, w_value, w_out,
    )


def solution(mesh):
    in_specs = (
        P("cp", "tp"),
        P(),
        P(None, "tp"),
        P(None, "tp"),
        P(None, "tp"),
        P("tp", None),
        P("cp"),
    )
    return jax.shard_map(
        sublayer, mesh=mesh, in_specs=in_specs, out_specs=P("cp", "tp"), check_vma=False
    )
```

```python
import math

import jax
import jax.numpy as jnp
from jax import lax
from jax.experimental import pallas as pl
from jax.experimental.pallas import tpu as pltpu
from jax.sharding import PartitionSpec as P

HEADS = 32
KV_HEADS = 8
HEAD_SIZE = 128
LONGEST = 12288
DOCS = 6
TOK = 512
GROUP = 4
ROWS = GROUP * TOK
BLK = 2 * TOK + 16
PENALTY = -(2.0**100)
SCALE = math.log2(math.e) / math.sqrt(HEAD_SIZE)
QC = 512

epsilon = 1e-05
rope_base = 500000.0


WIDTH = 4096
PIECE = 512
N_TP = 8
CH = 4
CR = TOK // CH
MESH = pl.DeviceIdType.MESH


def tp_places():
    t = lax.axis_index("tp")
    plane = (t // 4) * 4
    y = t % 4
    up = plane + (y + 1) % 4
    down = plane + (y + 3) % 4
    far = plane + (y + 2) % 4
    return t, up, down, far


def other(t):
    return (t + 4) % 8


def part(chunk):
    return pl.ds(chunk * CR, CR)


def projection(
    h_ref, gain_ref, doc_ref, weights, inputs, q_out, kv_out, begin,
    gath, w, acc, squares, cosine, sine, ssem, rsem, qssem, qrsem,
):
    t, up, down, far = tp_places()
    across = other(t)
    peers = [(t + i) % N_TP for i in range(1, N_TP)]
    for copy in inputs:
        copy.wait()
    sent = []

    def send(source, owner, chunk, to):
        copy = pltpu.make_async_remote_copy(
            src_ref=source,
            dst_ref=gath.at[owner, part(chunk)],
            send_sem=ssem.at[len(sent)],
            recv_sem=rsem.at[owner, chunk],
            device_id={"tp": to},
            device_id_type=MESH,
        )
        copy.start()
        sent.append(copy)

    def arrived(owner, chunk):
        pltpu.make_async_remote_copy(
            src_ref=gath.at[owner, part(chunk)],
            dst_ref=gath.at[owner, part(chunk)],
            send_sem=ssem.at[0],
            recv_sem=rsem.at[owner, chunk],
            device_id={"tp": across},
            device_id_type=MESH,
        ).wait_recv()

    upward = (0, 1, 2, 3)
    downward = (2, 3, 0, 1)

    def send_own(i):
        send(h_ref.at[part(upward[i])], t, upward[i], up)
        send(h_ref.at[part(downward[i])], t, downward[i], down)
        send(h_ref.at[part(upward[i])], t, upward[i], across)

    send_own(0)
    mine = h_ref[...].astype(jnp.float32)
    mass = jnp.sum(mine * mine, axis=1, keepdims=True)
    squares[t] = jnp.broadcast_to(mass, (TOK, 128)).T[0:8]
    told = []
    for i, peer in enumerate(peers):
        copy = pltpu.make_async_remote_copy(
            src_ref=squares.at[t],
            dst_ref=squares.at[t],
            send_sem=qssem.at[i],
            recv_sem=qrsem.at[t],
            device_id={"tp": peer},
            device_id_type=MESH,
        )
        copy.start()
        told.append(copy)
    for i in range(1, CH):
        send_own(i)

    first = lax.axis_index("cp") * TOK
    place = (first + lax.broadcasted_iota(jnp.int32, (HEAD_SIZE // 2, TOK), 1)).astype(jnp.float32)
    pair = lax.broadcasted_iota(jnp.int32, (HEAD_SIZE // 2, 128), 0)
    freqs = jnp.zeros((HEAD_SIZE // 2, 128), jnp.float32)
    for i in range(HEAD_SIZE // 2):
        freqs = jnp.where(pair == i, jnp.float32(rope_base ** (-2.0 * i / HEAD_SIZE)), freqs)
    angle = place * jnp.concatenate([freqs] * (TOK // 128), axis=1)
    cosine[...] = jnp.cos(angle)
    sine[...] = jnp.sin(angle)
    for peer in peers:
        pltpu.make_async_remote_copy(
            src_ref=squares.at[peer],
            dst_ref=squares.at[peer],
            send_sem=qssem.at[0],
            recv_sem=qrsem.at[peer],
            device_id={"tp": peer},
            device_id_type=MESH,
        ).wait_recv()
    whole = jnp.sum(squares[...], axis=0)[0:1]
    inverse = lax.rsqrt(whole / WIDTH + epsilon)
    inverse = jnp.broadcast_to(inverse, (128, TOK)).T
    inverse = jnp.concatenate([inverse] * (PIECE // 128), axis=1)
    for copy in weights:
        copy.wait()

    def use(source, owner, start):
        gain = gain_ref[:, pl.ds(pl.multiple_of(owner * PIECE, PIECE), PIECE)]
        normed = (source[...].astype(jnp.float32) * inverse * gain).astype(jnp.bfloat16)
        rows = pl.ds(pl.multiple_of(owner * PIECE, PIECE), PIECE)
        product = jnp.dot(normed, w[rows, :], preferred_element_type=jnp.float32)
        if start:
            acc[...] = product
        else:
            acc[...] += product

    use(h_ref, t, True)
    for i in range(CH):
        arrived(down, upward[i])
        if i < 2:
            send(gath.at[down, part(upward[i])], down, upward[i], up)
        arrived(up, downward[i])
        if i < 2:
            send(gath.at[up, part(downward[i])], up, downward[i], down)
        arrived(across, upward[i])
        if i == 1:
            for chunk in (0, 1):
                send(gath.at[across, part(chunk)], across, chunk, up)
                send(gath.at[across, part(chunk)], across, chunk, down)
        if i > 1:
            send(gath.at[across, part(i)], across, i, up)
            send(gath.at[across, part(i)], across, i, down)
    use(gath.at[up], up, False)
    use(gath.at[down], down, False)
    for i in range(2):
        for chunk in (upward[i], downward[i]):
            arrived(far, chunk)
            send(gath.at[far, part(chunk)], far, chunk, across)
    use(gath.at[across], across, False)
    use(gath.at[far], far, False)
    for chunk in (0, 2, 1, 3):
        arrived(other(far), chunk)
    use(gath.at[other(far)], other(far), False)
    for side in (up, down):
        for chunk in range(CH):
            arrived(other(side), chunk)
        use(gath.at[other(side)], other(side), False)

    half = HEAD_SIZE // 2

    def rotated(head):
        raw = acc[:, head * HEAD_SIZE : (head + 1) * HEAD_SIZE].T
        low = raw[:half] * cosine[...] - raw[half:] * sine[...]
        high = raw[half:] * cosine[...] + raw[:half] * sine[...]
        return low, high

    low, high = rotated(GROUP)
    kv_out[0:TOK, :] = jnp.concatenate([low, high], axis=0).T.astype(jnp.bfloat16)
    value = acc[:, (GROUP + 1) * HEAD_SIZE :].T.astype(jnp.bfloat16)
    for i in range(TOK // 128):
        kv_out[TOK + 128 * i : TOK + 128 * (i + 1), :] = value[:, 128 * i : 128 * (i + 1)]
    lane = lax.broadcasted_iota(jnp.int32, (16, 128), 1)
    row = lax.broadcasted_iota(jnp.int32, (16, 128), 0)
    tail = jnp.zeros((16, 128), jnp.int32)
    for d in range(1, DOCS):
        count = jnp.sum(jnp.where(doc_ref[...] < d, 1, 0), axis=1, keepdims=True)
        tail = jnp.where(
            (lane == d) & (row == 0), count // 16, jnp.where((lane == d) & (row == 1), count % 16, tail)
        )
    kv_out[2 * TOK :, :] = tail.astype(jnp.float32).astype(jnp.bfloat16)
    begin()
    for head in range(GROUP):
        low, high = rotated(head)
        cols = slice(head * TOK, (head + 1) * TOK)
        q_out[0:half, cols] = (low * SCALE).astype(jnp.bfloat16)
        q_out[half:HEAD_SIZE, cols] = (high * SCALE).astype(jnp.bfloat16)
    return sent + told


def combination(
    att, out_ref, weights, w, terms, sums, across_in, side_in, half_in, side_end, across_end, ssem, rsem,
):
    t, up, down, far = tp_places()
    across = other(t)
    sent = []

    def send(source, target, number, to):
        copy = pltpu.make_async_remote_copy(
            src_ref=source,
            dst_ref=target,
            send_sem=ssem.at[len(sent)],
            recv_sem=rsem.at[number],
            device_id={"tp": to},
            device_id_type=MESH,
        )
        copy.start()
        sent.append(copy)

    def arrived(target, number):
        pltpu.make_async_remote_copy(
            src_ref=target,
            dst_ref=target,
            send_sem=ssem.at[0],
            recv_sem=rsem.at[number],
            device_id={"tp": across},
            device_id_type=MESH,
        ).wait_recv()
        return target[...].astype(jnp.float32)

    def compute(i):
        weights[i].wait()
        product = jnp.dot(att[...], w[i], preferred_element_type=jnp.float32)
        terms[i] = product.astype(jnp.bfloat16)

    def term(i, chunk):
        return terms[i, part(chunk)].astype(jnp.float32)

    UP, DOWN = 0, 1
    compute(0)
    for chunk in (0, 2, 1, 3):
        send(terms.at[0, part(chunk)], across_in.at[part(chunk)], chunk, across)
    compute(1)
    compute(2)
    for chunk in range(CH):
        send(terms.at[1, part(chunk)], side_in.at[DOWN, part(chunk)], 4 + chunk, up)
        send(terms.at[2, part(chunk)], side_in.at[UP, part(chunk)], 8 + chunk, down)
    for i in range(3, 8):
        compute(i)
    for chunk in (0, 2, 1, 3):
        got = arrived(across_in.at[part(chunk)], chunk)
        sums[0, part(chunk)] = (term(3, chunk) + got).astype(jnp.bfloat16)
        if chunk < 2:
            send(sums.at[0, part(chunk)], half_in.at[DOWN, part(chunk)], 12 + chunk, up)
        else:
            send(sums.at[0, part(chunk)], half_in.at[UP, part(chunk - 2)], 12 + chunk, down)
    for chunk in range(CH):
        below = arrived(side_in.at[DOWN, part(chunk)], 4 + chunk)
        above = arrived(side_in.at[UP, part(chunk)], 8 + chunk)
        sums[1, part(chunk)] = (term(4, chunk) + below + above).astype(jnp.bfloat16)
        send(sums.at[1, part(chunk)], across_end.at[part(chunk)], 16 + chunk, across)
    for i in range(2):
        send(terms.at[5, part(2 + i)], side_end.at[DOWN, part(2 + i)], 22 + i, up)
        send(terms.at[6, part(i)], side_end.at[UP, part(i)], 24 + i, down)
    for i in range(2):
        got = arrived(half_in.at[DOWN, part(i)], 12 + i)
        sums[2, part(i)] = (term(5, i) + got).astype(jnp.bfloat16)
        send(sums.at[2, part(i)], side_end.at[DOWN, part(i)], 20 + i, up)
        got = arrived(half_in.at[UP, part(i)], 14 + i)
        sums[3, part(2 + i)] = (term(6, 2 + i) + got).astype(jnp.bfloat16)
        send(sums.at[3, part(2 + i)], side_end.at[UP, part(2 + i)], 26 + i, down)
    for chunk in range(CH):
        total = term(7, chunk) + arrived(across_end.at[part(chunk)], 16 + chunk)
        total = total + arrived(side_end.at[DOWN, part(chunk)], 20 + chunk)
        total = total + arrived(side_end.at[UP, part(chunk)], 24 + chunk)
        out_ref[part(chunk), :] = total.astype(jnp.bfloat16)
    return sent


def augment_queries(doc_ref, qaug):
    row = lax.broadcasted_iota(jnp.int32, (HEAD_SIZE, TOK), 0)
    hot = jnp.where(row == doc_ref[...], PENALTY, 0.0).astype(jnp.bfloat16)
    for head in range(GROUP):
        qaug[HEAD_SIZE:, head * TOK : (head + 1) * TOK] = hot


def attend_keys(block):
    counts = block[2 * TOK : 2 * TOK + 2, :].astype(jnp.float32)
    below = counts[0:1] * 16.0 + counts[1:2]
    row = lax.broadcasted_iota(jnp.int32, (TOK, HEAD_SIZE), 0).astype(jnp.float32)
    earlier = jnp.where(row < below, 1.0, 0.0).astype(jnp.bfloat16)
    return jnp.concatenate([block[0:TOK, :], earlier], axis=1)


def score(keys, chunk, slot, qaug, logits, tops, causal):
    cols = slice(chunk * QC, (chunk + 1) * QC)
    length = keys.shape[0]
    scores = jnp.dot(keys, qaug[:, cols], preferred_element_type=jnp.float32)
    if causal:
        key_at = lax.broadcasted_iota(jnp.int32, (TOK, QC), 0)
        query_at = lax.broadcasted_iota(jnp.int32, (TOK, QC), 1) + (chunk * QC) % TOK
        scores = jnp.where(key_at <= query_at, scores, jnp.float32(PENALTY))
    logits[slot, 0:length] = scores
    tops[slot] = jnp.max(scores, axis=0, keepdims=True)


def weigh(values, chunk, slot, logits, tops, best, acc, first):
    cols = slice(chunk * QC, (chunk + 1) * QC)
    top = tops[slot]
    if not first:
        old = best[:, cols]
        top = jnp.maximum(old, top)
    weights = jnp.exp2(logits[slot, 0 : values.shape[1]] - top).astype(jnp.bfloat16)
    out = jnp.dot(values, weights, preferred_element_type=jnp.float32)
    if first:
        acc[:, cols] = out
    else:
        acc[:, cols] = acc[:, cols] * jnp.exp2(old - top) + out
    best[:, cols] = top


def attend(blocks, state, first):
    qaug, logits, tops, best, acc = state
    chunks = ROWS // QC
    keys = jnp.concatenate([attend_keys(block) for block in blocks], axis=0)
    values = jnp.concatenate(
        [
            block[TOK + 128 * i : TOK + 128 * (i + 1), :]
            for block in blocks
            for i in range(TOK // 128)
        ],
        axis=1,
    )
    ones = jnp.ones((16, values.shape[1]), jnp.bfloat16)
    values = jnp.concatenate([values, ones], axis=0)
    score(keys, 0, 0, qaug, logits, tops, first)
    for chunk in range(chunks):
        if chunk + 1 < chunks:
            score(keys, chunk + 1, (chunk + 1) % 2, qaug, logits, tops, first)
        weigh(values, chunk, chunk % 2, logits, tops, best, acc, first)


def finish(acc, out_ref):
    for head in range(GROUP):
        cols = slice(head * TOK, (head + 1) * TOK)
        total = acc[HEAD_SIZE : HEAD_SIZE + 1, cols]
        out_ref[:, head * HEAD_SIZE : (head + 1) * HEAD_SIZE] = (
            (acc[0:HEAD_SIZE, cols] / total).T.astype(jnp.bfloat16)
        )


ROLES = 15
PARTS = ((0, TOK), (TOK, TOK + 16))
PROGRAM = [
    (0, [(0, 0), (0, 1), (15, 0), (15, 1)]),
    (2, [(2, 0), (2, 1), (3, 0), (4, 0)]),
    (1, [(1, 0), (1, 1), (3, 1), (4, 1)]),
    (3, []),
    (4, [(5, 0), (6, 0)]),
    (5, [(5, 1), (6, 1)]),
    (6, [(11, 0), (7, 0)]),
    (9, [(9, 0), (9, 1)]),
    (8, [(8, 0), (8, 1)]),
    (11, [(11, 1), (12, 0), (13, 0), (7, 1)]),
    (7, []),
    (12, [(12, 1), (13, 1)]),
    (13, [(10, 0), (10, 1)]),
    (10, [(14, 0), (14, 1)]),
    (14, []),
]


def attention(
    doc_ref, own_ref, out_ref, kv, qaug, logits, tops, best, acc, ssem, rsem, sibsend, sibrecv,
):
    me = lax.axis_index("cp")
    core = me % 2
    x = (me // 2) % 4
    z = me // 8
    state = (qaug, logits, tops, best, acc)

    def at(zz, xx):
        return (zz * 4 + xx) * 2 + core

    right = at(z, (x + 1) % 4)
    left = at(z, (x + 3) % 4)
    ahead = at((z + 1) % 4, x)
    behind = at((z + 3) % 4, x)
    sibling = me + 1 - 2 * core

    def move(source, slot, half, to, send_sem, recv_sem):
        rows = pl.ds(*PARTS[half])
        return pltpu.make_async_remote_copy(
            src_ref=source.at[rows],
            dst_ref=kv.at[slot, rows],
            send_sem=send_sem,
            recv_sem=recv_sem,
            device_id={"cp": to},
            device_id_type=MESH,
        )

    always = z >= 0
    top = z == 3
    one, two = z >= 1, z >= 2
    xm, xp, x2 = (x + 3) % 4, (x + 1) % 4, (x + 2) % 4
    roles = [
        (x >= 1, z, xm),
        (x == 3, z, xp),
        (x >= 2, z, x2),
        (one, (z + 3) % 4, x),
        (top, 0 * z, x),
        (one, (z + 3) % 4, xm),
        (one, (z + 3) % 4, xp),
        (top & (x < 3), 0 * z, xp),
        (top & (x == 0), 0 * z, xm),
        (one, (z + 3) % 4, x2),
        (top & (x < 2), 0 * z, x2),
        (two, (z + 2) % 4, x),
        (two, (z + 2) % 4, xm),
        (two, (z + 2) % 4, xp),
        (two, (z + 2) % 4, x2),
        ((z == 0) & (x < 3), z, xp),
    ]
    slots = [at(zz, xx) for _, zz, xx in roles]
    middle = (x == 1) | (x == 2)
    forwards = {
        0: [(middle, right, (0, 1))],
        3: [(z < 3, ahead, (0, 1)), (always, right, (0, 1)), (always, left, (1, 0))],
        4: [(x == 3, right, (0, 1))],
        5: [(always, right, (0,))],
        6: [(always, left, (1,))],
        7: [(middle, left, (0, 1))],
        15: [(always, behind, (0, 1))],
        11: [(always, right, (0, 1)), (always, left, (1, 0))],
        12: [(always, right, (0, 1))],
    }
    sends = []

    def plan(when, source, slot, half, to):
        number = len(sends)
        sends.append((when, source, slot, half, to))
        return number

    def issue(number):
        when, source, slot, half, to = sends[number]

        @pl.when(when)
        def _():
            move(source, slot, half, to, ssem.at[number], rsem.at[slot, half]).start()

    own = []
    for half in (0, 1):
        own.append(plan(z < 3, own_ref, me, half, ahead))
        own.append(plan(z == 0, own_ref, me, half, behind))
        own.append(plan(x < 3, own_ref, me, half, right))
        own.append(plan((x == 0) | (z == 0), own_ref, me, half, left))
    relays = {}
    for role, targets in forwards.items():
        relays[role] = {0: [], 1: []}
        for when, to, halves in targets:
            for half in halves:
                number = plan(roles[role][0] & when, kv.at[slots[role]], slots[role], half, to)
                relays[role][half].append(number)

    def begin():
        for number in own:
            issue(number)
        for half in (0, 1):
            move(own_ref, me, half, sibling, sibsend.at[ROLES, half], sibrecv.at[ROLES, half]).start()

    def serve(role, half):
        slot = slots[role]

        @pl.when(roles[role][0])
        def _():
            move(own_ref, slot, half, sibling, ssem.at[0], rsem.at[slot, half]).wait_recv()
            if role < ROLES:
                move(
                    kv.at[slot], slot, half, sibling, sibsend.at[role, half], sibrecv.at[role, half]
                ).start()

        for number in relays.get(role, {0: [], 1: []})[half]:
            issue(number)

    def run():
        augment_queries(doc_ref, qaug)
        attend([own_ref], state, True)
        for half in (0, 1):
            move(own_ref, sibling, half, sibling, sibsend.at[ROLES, half], sibrecv.at[ROLES, half]).wait_recv()

        @pl.when(core == 1)
        def _():
            attend([kv.at[sibling]], state, False)

        @pl.loop(0, ROLES)
        def _(step):
            there = step < 0
            slot = 0 * step
            turn = 0 * step
            for index, (role, services) in enumerate(PROGRAM):

                @pl.when(step == index)
                def _():
                    for service in services:
                        serve(*service)

                there = there | ((step == index) & roles[role][0])
                slot = jnp.where(step == index, slots[role], slot)
                turn = jnp.where(step == index, role, turn)

            @pl.when(there)
            def _():
                twin = slot + 1 - 2 * core
                for half in (0, 1):
                    move(own_ref, twin, half, sibling, sibsend.at[turn, half], sibrecv.at[turn, half]).wait_recv()
                attend([kv.at[slot], kv.at[twin]], state, False)

        finish(acc, out_ref)

    def drain():
        for number, (when, source, slot, half, to) in enumerate(sends):

            @pl.when(when)
            def _():
                move(source, slot, half, to, ssem.at[number], rsem.at[slot, half]).wait_send()

        for role in range(ROLES + 1):
            present, slot = (always, me) if role == ROLES else (roles[role][0], slots[role])
            for half in (0, 1):

                @pl.when(present)
                def _():
                    move(
                        own_ref, slot, half, sibling, sibsend.at[role, half], sibrecv.at[role, half]
                    ).wait_send()

    return begin, run, drain


SENDS = 30
BF16, F32 = jnp.bfloat16, jnp.float32


def fused_kernel(
    h_hbm, gain_hbm, doc_hbm, wq, wk, wv, w_out, out_ref,
    gath, w, pacc, squares, cosine, sine, gain_ref, doc_ref, insem, pssem, prsem, qssem, qrsem,
    own, kv, qaug, logits, tops, best, acc, assem, arsem, sibsend, sibrecv, att,
    wo, terms, sums, across_in, side_in, half_in, side_end, across_end, wosem, cssem, crsem,
):
    t, up, down, far = tp_places()
    across = other(t)
    me = lax.axis_index("cp")
    h_ref = gath.at[t]
    inputs = [
        pltpu.make_async_copy(h_hbm, h_ref, insem.at[0]),
        pltpu.make_async_copy(gain_hbm, gain_ref, insem.at[1]),
        pltpu.make_async_copy(doc_hbm, doc_ref, insem.at[2]),
    ]
    weights = [
        pltpu.make_async_copy(wq, w.at[:, 0:512], insem.at[3]),
        pltpu.make_async_copy(wk, w.at[:, 512:640], insem.at[4]),
        pltpu.make_async_copy(wv, w.at[:, 640:768], insem.at[5]),
    ]
    order = [other(far), other(up), other(down), far, across, up, down, t]
    late = []
    for i, owner in enumerate(order):
        cols = pl.ds(pl.multiple_of(owner * PIECE, PIECE), PIECE)
        late.append(pltpu.make_async_copy(w_out.at[:, cols], wo.at[i], wosem.at[i]))
    for copy in inputs + weights + late:
        copy.start()
    core = me % 2
    column = (me // 2) % 4
    row = me // 8
    barrier = pltpu.get_barrier_semaphore()
    around = [
        me - me % 8 + (me + 2) % 8,
        me - me % 8 + (me + 6) % 8,
        (me + 8) % 32,
        (me + 24) % 32,
        me + 1 - 2 * core,
    ]
    for i in range(1, N_TP):
        pl.semaphore_signal(barrier, inc=1, device_id={"tp": (t + i) % N_TP}, device_id_type=MESH)
    for peer in around:
        pl.semaphore_signal(barrier, inc=1, device_id={"cp": peer}, device_id_type=MESH)
    pl.semaphore_wait(barrier, N_TP - 1 + len(around))

    begin, run, drain = attention(
        doc_ref, own, att, kv, qaug, logits, tops, best, acc, assem, arsem, sibsend, sibrecv
    )
    sent = projection(
        h_ref, gain_ref, doc_ref, weights, inputs, qaug, own, begin,
        gath, w, pacc, squares, cosine, sine, pssem, prsem, qssem, qrsem,
    )
    run()
    sent += combination(
        att, out_ref, late, wo, terms, sums, across_in, side_in, half_in, side_end, across_end, cssem, crsem
    )
    drain()
    for copy in sent:
        copy.wait_send()


def sublayer(hidden, norm_gain, w_query, w_key, w_value, w_out, doc_ids):
    hbm = pl.BlockSpec(memory_space=pl.ANY)
    dma = pltpu.SemaphoreType.DMA
    return pl.pallas_call(
        fused_kernel,
        out_shape=jax.ShapeDtypeStruct((TOK, PIECE), BF16),
        in_specs=[hbm] * 7,
        out_specs=pl.BlockSpec(memory_space=pltpu.VMEM),
        scratch_shapes=[
            pltpu.VMEM((N_TP, TOK, PIECE), BF16),
            pltpu.VMEM((WIDTH, 768), BF16),
            pltpu.VMEM((TOK, 768), F32),
            pltpu.VMEM((N_TP, 8, TOK), F32),
            pltpu.VMEM((HEAD_SIZE // 2, TOK), F32),
            pltpu.VMEM((HEAD_SIZE // 2, TOK), F32),
            pltpu.VMEM((1, WIDTH), F32),
            pltpu.VMEM((1, TOK), jnp.int32),
            dma((6,)),
            dma((28,)),
            dma((N_TP, CH)),
            dma((N_TP - 1,)),
            dma((N_TP,)),
            pltpu.VMEM((BLK, 128), BF16),
            pltpu.VMEM((32, BLK, 128), BF16),
            pltpu.VMEM((2 * HEAD_SIZE, ROWS), BF16),
            pltpu.VMEM((2, 2 * TOK, QC), F32),
            pltpu.VMEM((2, 1, QC), F32),
            pltpu.VMEM((1, ROWS), F32),
            pltpu.VMEM((HEAD_SIZE + 16, ROWS), F32),
            dma((SENDS,)),
            dma((32, 2)),
            dma((ROLES + 1, 2)),
            dma((ROLES + 1, 2)),
            pltpu.VMEM((TOK, GROUP * HEAD_SIZE), BF16),
            pltpu.VMEM((N_TP, PIECE, PIECE), BF16),
            pltpu.VMEM((N_TP, TOK, PIECE), BF16),
            pltpu.VMEM((4, TOK, PIECE), BF16),
            pltpu.VMEM((TOK, PIECE), BF16),
            pltpu.VMEM((2, TOK, PIECE), BF16),
            pltpu.VMEM((2, TOK // 2, PIECE), BF16),
            pltpu.VMEM((2, TOK, PIECE), BF16),
            pltpu.VMEM((TOK, PIECE), BF16),
            dma((N_TP,)),
            dma((28,)),
            dma((28,)),
        ],
        compiler_params=pltpu.CompilerParams(
            collective_id=0, has_side_effects=True, vmem_limit_bytes=63 * 2**20
        ),
        name="sublayer",
    )(
        hidden, norm_gain.reshape(1, WIDTH), doc_ids.reshape(1, TOK),
        w_query, w_key, w_value, w_out,
    )


def solution(mesh):
    in_specs = (
        P("cp", "tp"),
        P(),
        P(None, "tp"),
        P(None, "tp"),
        P(None, "tp"),
        P("tp", None),
        P("cp"),
    )
    return jax.shard_map(
        sublayer, mesh=mesh, in_specs=in_specs, out_specs=P("cp", "tp"), check_vma=False
    )
```
